512 devices in a mesh: tok: 64 (over x, z), blk: 8 (over y, core).
Axes of the slice: x: 4, y: 4, z: 16, core: 2. Of those that a mesh axis runs over, the one named last changes fastest.
Arguments:
- activations: bfloat16 [16384, 2048], P('tok', 'blk'), may hold values from -16 to 16
Outputs:
- factored: float32 [2048, 2048], P('blk', 'tok')
The draws below stay inside these ranges and needn't reach their ends.
All inputs are finite; a program needn't handle non-finite values.
Results may differ from the reference program's by a relative error of at most 0.0003.
Values may be sent and summed in bfloat16 or wider, within the bound.
A program may use at most 64 MiB of HBM per device.

```python
import math
import jax
import jax.numpy as jnp
from jax import lax

D = 2048
STEPS = 4
TOKENS = 16384
N_TOK = 64


def draw_activations(key, part):
    first, second, third, fourth = jax.random.split(key, 4)
    scales = jnp.exp(jax.random.uniform(first, (D,), jnp.float32, math.log(0.3), math.log(3.0)))
    base = jax.random.normal(second, (TOKENS, D), jnp.float32)
    shared_weight = 0.6
    common = jax.random.normal(third, (TOKENS, 16), jnp.float32)
    mixing = jax.random.normal(fourth, (16, D), jnp.float32) * 0.25
    values = (base + shared_weight * jnp.dot(common, mixing)) * scales
    return jnp.clip(values, -16.0, 16.0).astype(jnp.bfloat16)


def setup_inputs(seed: int = 0) -> dict:
    key_of = jax.random.split(jax.random.key(seed), 2)
    return {
        "activations": draw_activations(jax.random.fold_in(key_of[1], 71), 0),
    }


def reference(activations):
    total = activations.shape[0]
    hessian = lax.dot_general(activations.astype(jnp.float32), activations.astype(jnp.float32), (((0,), (0,)), ((), ())), preferred_element_type=jnp.float32) * (2.0 / total)
    damping = 0.01 * jnp.mean(jnp.diagonal(hessian))
    damped = hessian + damping * jnp.eye(D, dtype=jnp.float32)
    cols = STEPS * (D // N_TOK)
    leading = jnp.linalg.cholesky(damped[:cols, :cols])
    lower = jax.scipy.linalg.solve_triangular(leading, damped[cols:, :cols].T, lower=True).T
    schur = damped[cols:, cols:] - jnp.dot(lower, lower.T, precision=lax.Precision.HIGHEST)
    left_part = jnp.concatenate([leading, lower], 0)
    right_part = jnp.concatenate([jnp.zeros((cols, D - cols), jnp.float32), jnp.tril(schur)], 0)
    return jnp.concatenate([left_part, right_part], 1)
```

```python
import jax
import jax.numpy as jnp
from jax import lax
from jax.experimental import pallas as pl
from jax.experimental.pallas import tpu as pltpu
from jax.sharding import Mesh
from jax.sharding import PartitionSpec as P

MESH = pl.DeviceIdType.MESH
F32 = jnp.float32
BF16 = jnp.bfloat16
NX, NZ, NY, NC = 4, 16, 4, 2
BLOCK = 256
PANEL = 128
SLICE = BLOCK // NX
FULL = BLOCK * NY * NC
TOKENS = BLOCK * NX * NZ
SCALE = 2.0 / TOKENS


def wait(ref, sem):
    pltpu.make_async_copy(ref, ref, sem).wait()


def send(src, dst, send_sem, recv_sem, device):
    pltpu.make_async_remote_copy(
        src_ref=src,
        dst_ref=dst,
        send_sem=send_sem,
        recv_sem=recv_sem,
        device_id=device,
        device_id_type=MESH,
    ).start()


def exchange(a_ref, f_out, rows_out, cols_out, pivot_out, trace_out, feats, slices, partial, inbox, total, tall,
             rows, cols, pivot, owned, tz, ty, tq, tr,
             g1_s, g1_r, sib_s, sib_r, sl_s, sl_r, z_s, z_r, tz_s, tz_r, ty_s, ty_r, p1_s, p1_r,
             rows_s, rows_r, cols_s, cols_r, piv_s, piv_r, own_s, own_r):
    x, z, y, c = (lax.axis_index(name) for name in ("x", "z", "y", "c"))
    other = 1 - c
    mine = pl.ds(pl.multiple_of(x * SLICE, SLICE), SLICE)

    feats[c, x] = a_ref[...].T
    for d in (1, 3, 2):
        send(feats.at[c, x], feats.at[c, x], g1_s.at[d], g1_r.at[x], (lax.rem(x + d, NX), z, y, c))

    def relay(piece):
        send(feats.at[c, piece], feats.at[c, piece], sib_s.at[piece], sib_r.at[piece], (x, z, y, other))
        for target in range(1, NY):
            @pl.when(target > y)
            def _():
                send(feats.at[c, piece, mine], slices.at[y, piece], sl_s.at[target, piece], sl_r.at[y, piece],
                     (x, z, target, c))
        slices[y, piece] = feats[c, piece, mine]

    relay(x)
    for d in (1, 3, 2):
        piece = lax.rem(x + d, NX)
        wait(feats.at[c, piece], g1_r.at[piece])
        relay(piece)
    for piece in range(NX):
        wait(feats.at[other, piece], sib_r.at[piece])

    for source in range(NY):
        @pl.when(source <= y)
        def _():
            @pl.when(source < y)
            def _():
                for piece in range(NX):
                    wait(slices.at[source, piece], sl_r.at[source, piece])
            for half in range(NC):
                acc = jnp.zeros((SLICE, BLOCK), F32)
                for piece in range(NX):
                    acc += lax.dot_general(slices[source, piece], feats[half, piece], (((1,), (1,)), ((), ())),
                                           preferred_element_type=F32)
                for s in range(SLICE // 8):
                    partial[source, NC * s + half] = acc[8 * s:8 * s + 8]

            @pl.loop(1, NZ)
            def _(d):
                target = lax.rem(z + d, NZ)
                send(partial.at[source, target], inbox.at[source, z], z_s.at[source], z_r.at[source], (x, target, y, c))
            pltpu.make_async_copy(partial.at[source, z], inbox.at[source, z], z_r.at[source]).start()
        if source == 0:
            acc = jnp.zeros((8, 128), F32)
            for half in range(NC):
                for piece in range(NX):
                    v = feats[half, piece].astype(F32)
                    v = jnp.sum((v * v).reshape(BLOCK // 8, 8, BLOCK), axis=0)
                    acc += v[:, :128] + v[:, 128:]
            tq[...] = acc

            @pl.loop(1, NZ)
            def _(d):
                target = lax.rem(z + d, NZ)
                send(tq, tz.at[z], tz_s, tz_r, (x, target, y, c))
            pltpu.make_async_copy(tq, tz.at[z], tz_r).start()

    panel = jnp.logical_and(x < 2, c == 0)
    zs, zc = z // NC, lax.rem(z, NC)
    wait(inbox.at[0], z_r.at[0])
    total[0] = jnp.sum(inbox[0], axis=0)

    @pl.when(panel)
    def _():
        @pl.loop(1, NZ)
        def _(d):
            target = lax.rem(z + d, NZ)
            send(total.at[0], tall.at[zc, zs], p1_s, p1_r, (x, target, y, c))
        pltpu.make_async_copy(total.at[0], tall.at[zc, zs], p1_r).start()

    wait(tz, tz_r)
    tr[...] = jnp.sum(tz[...], axis=0)

    @pl.loop(1, NY)
    def _(d):
        send(tr, ty.at[y], ty_s, ty_r, (x, z, lax.rem(y + d, NY), c))
    pltpu.make_async_copy(tr, ty.at[y], ty_r).start()

    def to_owner(source):
        owner_z = 8 * c + 2 * x + zs // 4
        local = jnp.logical_and(jnp.logical_and(source == x, owner_z == z), zc == c)
        slot = owned.at[lax.rem(zs, 4)]

        @pl.when(jnp.logical_not(local))
        def _():
            send(total.at[source], slot, own_s.at[source], own_r, (source, owner_z, y, zc))

        @pl.when(local)
        def _():
            pltpu.make_async_copy(total.at[source], slot, own_r).start()

    def owner_sent(source):
        owner_z = 8 * c + 2 * x + zs // 4
        local = jnp.logical_and(jnp.logical_and(source == x, owner_z == z), zc == c)

        @pl.when(jnp.logical_not(local))
        def _():
            wait(total.at[source], own_s.at[source])

    to_owner(0)
    for source in range(1, NY):
        @pl.when(source <= y)
        def _():
            wait(inbox.at[source], z_r.at[source])
            total[source] = jnp.sum(inbox[source], axis=0)
            to_owner(source)

    col_half = z // 8
    col_lanes = pl.ds(pl.multiple_of(lax.rem(z, 8) // 4 * 128, 128), 128)

    def spread(src, dst, sems, recv, count, place):
        @pl.loop(0, count)
        def _(i):
            tx, ty_, tc = place(i)
            here = jnp.logical_and(jnp.logical_and(tx == x, ty_ == y), tc == c)

            @pl.when(here)
            def _():
                pltpu.make_async_copy(src, dst, recv).start()

            @pl.when(jnp.logical_not(here))
            def _():
                send(src, dst, sems.at[i], recv, (tx, z, ty_, tc))

    def spread_done(src, sems, count, place):
        @pl.loop(0, count)
        def _(i):
            tx, ty_, tc = place(i)
            here = jnp.logical_and(jnp.logical_and(tx == x, ty_ == y), tc == c)

            @pl.when(jnp.logical_not(here))
            def _():
                wait(src, sems.at[i])

    def place_pivot(i):
        return i // 8, lax.rem(i // 2, NY), lax.rem(i, NC)

    def place_cols(i):
        return y, i // 2, lax.rem(i, NC)

    def place_rows(half):
        return lambda i: (i, y, half)

    pivot_src = tall.at[0, :, :, pl.ds(0, 128)]
    cols_src = tall.at[col_half, :, :, col_lanes]

    @pl.when(panel)
    def _():
        wait(tall, p1_r)

        @pl.when(y == 0)
        def _():
            spread(pivot_src, pivot.at[x], piv_s, piv_r, 32, place_pivot)
        spread(cols_src, cols.at[x], cols_s, cols_r, 8, place_cols)
        for half in range(NC):
            spread(tall.at[half], rows.at[x], rows_s.at[half], rows_r, NX, place_rows(half))

    wait(pivot, piv_r)
    wait(cols, cols_r)
    wait(rows, rows_r)
    wait(ty, ty_r)
    pivot_out[...] = pivot[...].reshape(PANEL, PANEL)
    cols_out[...] = cols[...].reshape(PANEL, PANEL)
    rows_out[...] = rows[...].reshape(PANEL, BLOCK)
    trace_out[...] = jnp.sum(ty[...], axis=0)

    @pl.when(x <= y)
    def _():
        wait(owned, own_r)
    f_out[...] = owned[...].reshape(32, BLOCK)

    for d in (1, 3, 2):
        wait(feats.at[c, x], g1_s.at[d])
    for piece in range(NX):
        wait(feats.at[c, piece], sib_s.at[piece])
        for target in range(1, NY):
            @pl.when(target > y)
            def _():
                wait(slices.at[y, piece], sl_s.at[target, piece])
    owner_sent(0)
    wait(partial.at[0, pl.ds(0, NZ - 1)], z_s.at[0])
    for source in range(1, NY):
        @pl.when(source <= y)
        def _():
            wait(partial.at[source, pl.ds(0, NZ - 1)], z_s.at[source])
            owner_sent(source)
    wait(tz.at[pl.ds(0, NZ - 1)], tz_s)
    wait(ty.at[pl.ds(0, NY - 1)], ty_s)

    @pl.when(panel)
    def _():
        for _ in range(1):
            wait(inbox.at[0, pl.ds(0, NZ - 1)], p1_s)

        @pl.when(y == 0)
        def _():
            spread_done(pivot_src, piv_s, 32, place_pivot)
        spread_done(cols_src, cols_s, 8, place_cols)
        for half in range(NC):
            spread_done(tall.at[half], rows_s.at[half], NX, place_rows(half))


def gathered(a):
    dma = pltpu.SemaphoreType.DMA
    vmem = pl.BlockSpec(memory_space=pltpu.VMEM)
    return pl.pallas_call(
        exchange,
        out_shape=[
            jax.ShapeDtypeStruct((32, BLOCK), F32),
            jax.ShapeDtypeStruct((PANEL, BLOCK), F32),
            jax.ShapeDtypeStruct((PANEL, PANEL), F32),
            jax.ShapeDtypeStruct((PANEL, PANEL), F32),
            jax.ShapeDtypeStruct((8, 128), F32),
        ],
        in_specs=[vmem],
        out_specs=[vmem] * 5,
        scratch_shapes=[
            pltpu.VMEM((NC, NX, BLOCK, BLOCK), BF16),
            pltpu.VMEM((NY, NX, SLICE, BLOCK), BF16),
            pltpu.VMEM((NY, NZ, 8, BLOCK), F32),
            pltpu.VMEM((NY, NZ, 8, BLOCK), F32),
            pltpu.VMEM((NY, 8, BLOCK), F32),
            pltpu.VMEM((NC, 8, 8, BLOCK), F32),
            pltpu.VMEM((2, 8, 8, BLOCK), F32),
            pltpu.VMEM((2, 8, 8, 128), F32),
            pltpu.VMEM((2, 8, 8, 128), F32),
            pltpu.VMEM((4, 8, BLOCK), F32),
            pltpu.VMEM((NZ, 8, 128), F32),
            pltpu.VMEM((NY, 8, 128), F32),
            pltpu.VMEM((8, 128), F32),
            pltpu.VMEM((8, 128), F32),
            dma((NX,)), dma((NX,)),
            dma((NX,)), dma((NX,)),
            dma((NY, NX)), dma((NY, NX)),
            dma((NY,)), dma((NY,)),
            dma(()), dma(()),
            dma(()), dma(()),
            dma(()), dma(()),
            dma((NC, NX)), dma(()),
            dma((8,)), dma(()),
            dma((32,)), dma(()),
            dma((NY,)), dma(()),
        ],
        compiler_params=pltpu.CompilerParams(has_side_effects=True),
    )(a)


def finish(f_ref, rows_ref, cols_ref, pivot_ref, trace_ref, out_ref, both):
    x, z, y, c = (lax.axis_index(name) for name in ("x", "z", "y", "c"))
    damp = jnp.sum(trace_ref[...], keepdims=True) * (SCALE * 0.01 / FULL)
    lane = lax.broadcasted_iota(jnp.int32, (8, PANEL), 1)
    sub = lax.broadcasted_iota(jnp.int32, (8, PANEL), 0)
    groups = []
    for g in range(PANEL // 8):
        diag = lane == sub + 8 * g
        left = pivot_ref[8 * g:8 * g + 8, :] * SCALE + jnp.where(diag, damp, 0.0)
        groups.append([left, jnp.where(diag, 1.0, 0.0).astype(F32)])
    for k in range(PANEL):
        g0, r0 = k // 8, k % 8
        left, right = groups[g0][0][r0:r0 + 1], groups[g0][1][r0:r0 + 1]
        inv = 1.0 / left[:, k:k + 1]
        left, right = left * inv, right * inv
        for g in range(g0, PANEL // 8):
            mult = groups[g][0][:, k:k + 1]
            if g == g0:
                if r0 == 7:
                    continue
                mult = jnp.where(sub[:, :1] > r0, mult, 0.0)
            groups[g] = [groups[g][0] - mult * left, groups[g][1] - mult * right]
    for g in range(PANEL // 8):
        diag = jnp.sum(jnp.where(lane == sub + 8 * g, groups[g][0], 0.0), axis=1, keepdims=True)
        both[8 * g:8 * g + 8, :] = groups[g][1] * lax.rsqrt(diag)
    inverse = both[...]
    ids = lax.broadcasted_iota(jnp.int32, (PANEL, BLOCK), 0)
    row0 = (y * NC + c) * BLOCK
    row_ids = row0 + lax.broadcasted_iota(jnp.int32, (PANEL, BLOCK), 1)
    rows = rows_ref[...] * SCALE + jnp.where(ids == row_ids, damp, 0.0)
    highest = lax.Precision.HIGHEST
    rows = jnp.dot(inverse, rows, precision=highest, preferred_element_type=F32)
    cols = jnp.dot(inverse, cols_ref[...] * SCALE, precision=highest, preferred_element_type=F32)
    both_rows = lax.dot_general(cols, rows, (((0,), (0,)), ((), ())), precision=highest, preferred_element_type=F32)
    strip0 = (x * NZ + z) * 32
    leading = strip0 < PANEL
    picked = jnp.where(leading, rows, both_rows)
    wide = jnp.zeros((32, BLOCK), F32)
    for q in range(4):
        wide = jnp.where(lax.rem(z, 4) == q, picked[32 * q:32 * q + 32], wide)
    col_ids = strip0 + lax.broadcasted_iota(jnp.int32, (32, BLOCK), 0)
    row_ids = row0 + lax.broadcasted_iota(jnp.int32, (32, BLOCK), 1)
    schur = f_ref[...] * SCALE + jnp.where(col_ids == row_ids, damp, 0.0) - wide
    wide = jnp.where(leading, wide, schur)
    out_ref[...] = jnp.where(row_ids >= col_ids, wide, 0.0).T


def shards(a):
    parts = gathered(a)
    vmem = pl.BlockSpec(memory_space=pltpu.VMEM)
    return pl.pallas_call(
        finish,
        out_shape=jax.ShapeDtypeStruct((BLOCK, 32), F32),
        in_specs=[vmem] * 5,
        out_specs=vmem,
        scratch_shapes=[pltpu.VMEM((PANEL, PANEL), F32)],
    )(*parts)


def solution(mesh):
    finer = Mesh(mesh.devices.reshape(NX, NZ, NY, NC), ("x", "z", "y", "c"))
    return jax.shard_map(
        shards, mesh=finer, in_specs=(P(("x", "z"), ("y", "c")),), out_specs=P(("y", "c"), ("x", "z")), check_vma=False
    )
```

```python
import jax
import jax.numpy as jnp
from jax import lax
from jax.experimental import pallas as pl
from jax.experimental.pallas import tpu as pltpu
from jax.sharding import Mesh
from jax.sharding import PartitionSpec as P

MESH = pl.DeviceIdType.MESH
F32 = jnp.float32
BF16 = jnp.bfloat16
NX, NZ, NY, NC = 4, 16, 4, 2
BLOCK = 256
PANEL = 128
SLICE = BLOCK // NX
FULL = BLOCK * NY * NC
TOKENS = BLOCK * NX * NZ
SCALE = 2.0 / TOKENS


def wait(ref, sem):
    pltpu.make_async_copy(ref, ref, sem).wait()


def send(src, dst, send_sem, recv_sem, device):
    pltpu.make_async_remote_copy(
        src_ref=src,
        dst_ref=dst,
        send_sem=send_sem,
        recv_sem=recv_sem,
        device_id=device,
        device_id_type=MESH,
    ).start()


def eliminate(groups, first, last, sub):
    for k in range(first, last):
        g0, r0 = k // 8, k % 8
        left, right = groups[g0][0][r0:r0 + 1], groups[g0][1][r0:r0 + 1]
        inv = 1.0 / left[:, k:k + 1]
        left, right = left * inv, right * inv
        for g in range(g0, PANEL // 8):
            mult = groups[g][0][:, k:k + 1]
            if g == g0:
                if r0 == 7:
                    continue
                mult = jnp.where(sub[:, :1] > r0, mult, 0.0)
            groups[g] = [groups[g][0] - mult * left, groups[g][1] - mult * right]


def exchange(a_ref, out_ref, feats, slices, partial, inbox, total, tall,
             rows, cols, pivot, owned, tz, ty, tq, tr, square,
             g1_s, g1_r, sib_s, sib_r, sl_s, sl_r, z_s, z_r, tz_s, tz_r, ty_s, ty_r, p1_s, p1_r,
             rows_s, rows_r, cols_s, cols_r, piv_s, piv_r, own_s, own_r):
    x, z, y, c = (lax.axis_index(name) for name in ("x", "z", "y", "c"))
    other = 1 - c
    mine = pl.ds(pl.multiple_of(x * SLICE, SLICE), SLICE)

    barrier = pltpu.get_barrier_semaphore()

    @pl.loop(1, NX * NY * NC)
    def _(i):
        there = (lax.rem(x + i // (NY * NC), NX), z, lax.rem(y + i // NC, NY), lax.rem(c + i, NC))
        pl.semaphore_signal(barrier, inc=1, device_id=there, device_id_type=MESH)

    @pl.loop(1, NZ)
    def _(d):
        there = (x, lax.rem(z + d, NZ), y, c)
        pl.semaphore_signal(barrier, inc=1, device_id=there, device_id_type=MESH)

    feats[c, x] = a_ref[...].T
    pl.semaphore_wait(barrier, NX * NY * NC - 1 + NZ - 1)
    for d in (1, 3, 2):
        send(feats.at[c, x], feats.at[c, x], g1_s.at[d], g1_r.at[x], (lax.rem(x + d, NX), z, y, c))

    def relay(piece):
        send(feats.at[c, piece], feats.at[c, piece], sib_s.at[piece], sib_r.at[piece], (x, z, y, other))
        for target in range(1, NY):
            @pl.when(target > y)
            def _():
                send(feats.at[c, piece, mine], slices.at[y, piece], sl_s.at[target, piece], sl_r.at[y, piece],
                     (x, z, target, c))
        slices[y, piece] = feats[c, piece, mine]

    relay(x)
    for d in (1, 3, 2):
        piece = lax.rem(x + d, NX)
        wait(feats.at[c, piece], g1_r.at[piece])
        relay(piece)
    for piece in range(NX):
        wait(feats.at[other, piece], sib_r.at[piece])

    def multiply(source):
        for half in range(NC):
            acc = jnp.zeros((SLICE, BLOCK), F32)
            for piece in range(NX):
                acc += lax.dot_general(slices[source, piece], feats[half, piece], (((1,), (1,)), ((), ())),
                                       preferred_element_type=F32)
            for s in range(SLICE // 8):
                partial[source, NC * s + half] = acc[8 * s:8 * s + 8]

    def reduce_to_peers(source):
        @pl.loop(1, NZ)
        def _(d):
            target = lax.rem(z + d, NZ)
            send(partial.at[source, target], inbox.at[source, z], z_s.at[source], z_r.at[source], (x, target, y, c))
        pltpu.make_async_copy(partial.at[source, z], inbox.at[source, z], z_r.at[source]).start()

    def arrived(source):
        @pl.when(source < y)
        def _():
            for piece in range(NX):
                wait(slices.at[source, piece], sl_r.at[source, piece])

    panel = jnp.logical_and(x < 2, c == 0)
    zs, zc = z // NC, lax.rem(z, NC)

    arrived(0)
    multiply(0)
    reduce_to_peers(0)
    acc = jnp.zeros((8, 128), F32)
    for half in range(NC):
        for piece in range(NX):
            v = feats[half, piece].astype(F32)
            v = jnp.sum((v * v).reshape(BLOCK // 8, 8, BLOCK), axis=0)
            acc += v[:, :128] + v[:, 128:]
    tq[...] = acc

    @pl.loop(1, NZ)
    def _(d):
        target = lax.rem(z + d, NZ)
        send(tq, tz.at[z], tz_s, tz_r, (x, target, y, c))
    pltpu.make_async_copy(tq, tz.at[z], tz_r).start()

    for source in range(1, NY):
        @pl.when(source <= y)
        def _():
            arrived(source)
            multiply(source)

            @pl.when(x >= 2)
            def _():
                reduce_to_peers(source)

    wait(inbox.at[0], z_r.at[0])
    total[0] = jnp.sum(inbox[0], axis=0)

    @pl.when(panel)
    def _():
        @pl.loop(1, NZ)
        def _(d):
            target = lax.rem(z + d, NZ)
            send(total.at[0], tall.at[zc, zs], p1_s, p1_r, (x, target, y, c))
        pltpu.make_async_copy(total.at[0], tall.at[zc, zs], p1_r).start()

    wait(tz, tz_r)
    tr[...] = jnp.sum(tz[...], axis=0)

    @pl.loop(1, NY)
    def _(d):
        send(tr, ty.at[y], ty_s, ty_r, (x, z, lax.rem(y + d, NY), c))
    pltpu.make_async_copy(tr, ty.at[y], ty_r).start()

    @pl.when(x < 2)
    def _():
        for source in range(1, NY):
            @pl.when(source <= y)
            def _():
                reduce_to_peers(source)

    def to_owner(source):
        owner_z = 8 * c + 2 * x + zs // 4
        local = jnp.logical_and(jnp.logical_and(source == x, owner_z == z), zc == c)
        slot = owned.at[lax.rem(zs, 4)]

        @pl.when(jnp.logical_not(local))
        def _():
            send(total.at[source], slot, own_s.at[source], own_r, (source, owner_z, y, zc))

        @pl.when(local)
        def _():
            pltpu.make_async_copy(total.at[source], slot, own_r).start()

    def owner_sent(source):
        owner_z = 8 * c + 2 * x + zs // 4
        local = jnp.logical_and(jnp.logical_and(source == x, owner_z == z), zc == c)

        @pl.when(jnp.logical_not(local))
        def _():
            wait(total.at[source], own_s.at[source])

    to_owner(0)

    col_half = z // 8
    col_lanes = pl.ds(pl.multiple_of(lax.rem(z, 8) // 4 * 128, 128), 128)

    def spread(src, dst, sems, recv, count, place):
        @pl.loop(0, count)
        def _(i):
            tx, ty_, tc = place(i)
            here = jnp.logical_and(jnp.logical_and(tx == x, ty_ == y), tc == c)

            @pl.when(here)
            def _():
                pltpu.make_async_copy(src, dst, recv).start()

            @pl.when(jnp.logical_not(here))
            def _():
                send(src, dst, sems.at[i], recv, (tx, z, ty_, tc))

    def spread_done(src, sems, count, place):
        @pl.loop(0, count)
        def _(i):
            tx, ty_, tc = place(i)
            here = jnp.logical_and(jnp.logical_and(tx == x, ty_ == y), tc == c)

            @pl.when(jnp.logical_not(here))
            def _():
                wait(src, sems.at[i])

    def place_pivot(i):
        return i // 8, lax.rem(i // 2, NY), lax.rem(i, NC)

    def place_cols(i):
        return y, i // 2, lax.rem(i, NC)

    def place_rows(half):
        return lambda i: (i, y, half)

    pivot_src = tall.at[0, :, :, pl.ds(0, 128)]
    cols_src = tall.at[col_half, :, :, col_lanes]

    @pl.when(panel)
    def _():
        wait(tall, p1_r)

        @pl.when(y == 0)
        def _():
            spread(pivot_src, pivot.at[x], piv_s, piv_r, 32, place_pivot)
        spread(cols_src, cols.at[x], cols_s, cols_r, 8, place_cols)
        for half in range(NC):
            spread(tall.at[half], rows.at[x], rows_s.at[half], rows_r, NX, place_rows(half))

    wait(pivot, piv_r)
    wait(ty, ty_r)
    damp = jnp.sum(jnp.sum(ty[...], axis=0), keepdims=True) * (SCALE * 0.01 / FULL)
    lane = lax.broadcasted_iota(jnp.int32, (8, PANEL), 1)
    sub = lax.broadcasted_iota(jnp.int32, (8, PANEL), 0)
    groups = []
    for g in range(PANEL // 8):
        diag = lane == sub + 8 * g
        left = pivot[g // 8, g % 8] * SCALE + jnp.where(diag, damp, 0.0)
        groups.append([left, jnp.where(diag, 1.0, 0.0).astype(F32)])
    eliminate(groups, 0, PANEL // 2, sub)
    for g in range(PANEL // 8):
        square[g, 0] = groups[g][0]
        square[g, 1] = groups[g][1]
    for source in range(1, NY):
        @pl.when(source <= y)
        def _():
            wait(inbox.at[source], z_r.at[source])
            total[source] = jnp.sum(inbox[source], axis=0)
            to_owner(source)
    groups = [[square[g, 0], square[g, 1]] for g in range(PANEL // 8)]
    eliminate(groups, PANEL // 2, PANEL, sub)
    scaled = []
    for g in range(PANEL // 8):
        diag = jnp.sum(jnp.where(lane == sub + 8 * g, groups[g][0], 0.0), axis=1, keepdims=True)
        scaled.append(groups[g][1] * lax.rsqrt(diag))
    inverse = jnp.concatenate(scaled, axis=0)
    wait(cols, cols_r)
    wait(rows, rows_r)
    ids = lax.broadcasted_iota(jnp.int32, (PANEL, BLOCK), 0)
    row0 = (y * NC + c) * BLOCK
    row_ids = row0 + lax.broadcasted_iota(jnp.int32, (PANEL, BLOCK), 1)
    right = rows[...].reshape(PANEL, BLOCK) * SCALE + jnp.where(ids == row_ids, damp, 0.0)
    highest = lax.Precision.HIGHEST
    right = jnp.dot(inverse, right, precision=highest, preferred_element_type=F32)
    left = jnp.dot(inverse, cols[...].reshape(PANEL, PANEL) * SCALE, precision=highest, preferred_element_type=F32)
    update = lax.dot_general(left, right, (((0,), (0,)), ((), ())), precision=highest, preferred_element_type=F32)
    strip0 = (x * NZ + z) * 32
    leading = strip0 < PANEL
    picked = jnp.where(leading, right, update)
    wide = jnp.zeros((32, BLOCK), F32)
    for q in range(4):
        wide = jnp.where(lax.rem(z, 4) == q, picked[32 * q:32 * q + 32], wide)
    col_ids = strip0 + lax.broadcasted_iota(jnp.int32, (32, BLOCK), 0)
    row_ids = row0 + lax.broadcasted_iota(jnp.int32, (32, BLOCK), 1)

    @pl.when(x <= y)
    def _():
        wait(owned, own_r)
    schur = owned[...].reshape(32, BLOCK) * SCALE + jnp.where(col_ids == row_ids, damp, 0.0) - wide
    wide = jnp.where(leading, wide, schur)
    out_ref[...] = jnp.where(row_ids >= col_ids, wide, 0.0)

    for d in (1, 3, 2):
        wait(feats.at[c, x], g1_s.at[d])
    for piece in range(NX):
        wait(feats.at[c, piece], sib_s.at[piece])
        for target in range(1, NY):
            @pl.when(target > y)
            def _():
                wait(slices.at[y, piece], sl_s.at[target, piece])
    owner_sent(0)
    wait(partial.at[0, pl.ds(0, NZ - 1)], z_s.at[0])
    for source in range(1, NY):
        @pl.when(source <= y)
        def _():
            wait(partial.at[source, pl.ds(0, NZ - 1)], z_s.at[source])
            owner_sent(source)
    wait(tz.at[pl.ds(0, NZ - 1)], tz_s)
    wait(ty.at[pl.ds(0, NY - 1)], ty_s)

    @pl.when(panel)
    def _():
        for _ in range(1):
            wait(inbox.at[0, pl.ds(0, NZ - 1)], p1_s)

        @pl.when(y == 0)
        def _():
            spread_done(pivot_src, piv_s, 32, place_pivot)
        spread_done(cols_src, cols_s, 8, place_cols)
        for half in range(NC):
            spread_done(tall.at[half], rows_s.at[half], NX, place_rows(half))


def gathered(a):
    dma = pltpu.SemaphoreType.DMA
    vmem = pl.BlockSpec(memory_space=pltpu.VMEM)
    return pl.pallas_call(
        exchange,
        out_shape=jax.ShapeDtypeStruct((32, BLOCK), F32),
        in_specs=[vmem],
        out_specs=vmem,
        scratch_shapes=[
            pltpu.VMEM((NC, NX, BLOCK, BLOCK), BF16),
            pltpu.VMEM((NY, NX, SLICE, BLOCK), BF16),
            pltpu.VMEM((NY, NZ, 8, BLOCK), F32),
            pltpu.VMEM((NY, NZ, 8, BLOCK), F32),
            pltpu.VMEM((NY, 8, BLOCK), F32),
            pltpu.VMEM((NC, 8, 8, BLOCK), F32),
            pltpu.VMEM((2, 8, 8, BLOCK), F32),
            pltpu.VMEM((2, 8, 8, 128), F32),
            pltpu.VMEM((2, 8, 8, 128), F32),
            pltpu.VMEM((4, 8, BLOCK), F32),
            pltpu.VMEM((NZ, 8, 128), F32),
            pltpu.VMEM((NY, 8, 128), F32),
            pltpu.VMEM((8, 128), F32),
            pltpu.VMEM((8, 128), F32),
            pltpu.VMEM((PANEL // 8, 2, 8, PANEL), F32),
            dma((NX,)), dma((NX,)),
            dma((NX,)), dma((NX,)),
            dma((NY, NX)), dma((NY, NX)),
            dma((NY,)), dma((NY,)),
            dma(()), dma(()),
            dma(()), dma(()),
            dma(()), dma(()),
            dma((NC, NX)), dma(()),
            dma((8,)), dma(()),
            dma((32,)), dma(()),
            dma((NY,)), dma(()),
        ],
        compiler_params=pltpu.CompilerParams(collective_id=0, has_side_effects=True),
    )(a)


def shards(a):
    return gathered(a).T


def solution(mesh):
    finer = Mesh(mesh.devices.reshape(NX, NZ, NY, NC), ("x", "z", "y", "c"))
    return jax.shard_map(
        shards, mesh=finer, in_specs=(P(("x", "z"), ("y", "c")),), out_specs=P(("y", "c"), ("x", "z")), check_vma=False
    )
```

```python
import jax
import jax.numpy as jnp
from jax import lax
from jax.experimental import pallas as pl
from jax.experimental.pallas import tpu as pltpu
from jax.sharding import Mesh
from jax.sharding import PartitionSpec as P

MESH = pl.DeviceIdType.MESH
F32 = jnp.float32
BF16 = jnp.bfloat16
NX, NZ, NY, NC = 4, 16, 4, 2
BLOCK = 256
PANEL = 128
SLICE = BLOCK // NX
FULL = BLOCK * NY * NC
TOKENS = BLOCK * NX * NZ
SCALE = 2.0 / TOKENS


def wait(ref, sem):
    pltpu.make_async_copy(ref, ref, sem).wait()


def send(src, dst, send_sem, recv_sem, device):
    pltpu.make_async_remote_copy(
        src_ref=src,
        dst_ref=dst,
        send_sem=send_sem,
        recv_sem=recv_sem,
        device_id=device,
        device_id_type=MESH,
    ).start()


def spread_rows(row):
    return jnp.broadcast_to(row, (8, PANEL))


def spread_lane(tile, lane):
    return jnp.broadcast_to(tile[:, lane:lane + 1], (8, PANEL))


def eliminate(groups, first, last, sub):
    for k in range(first, last, 4):
        g0, r0 = k // 8, k % 8
        head = groups[g0]
        rows = [[spread_rows(head[h][r0 + i:r0 + i + 1]) for h in range(2)] for i in range(4)]
        dots = [[spread_lane(rows[i][0], k + j) if j >= i else None for j in range(4)] for i in range(4)]
        mults = [[None] * 4 for _ in range(4)]
        scaled = []
        for i in range(4):
            inv = 1.0 / dots[i][i]
            for j in range(i + 1, 4):
                mults[i][j] = dots[i][j] * inv
            for j in range(i + 1, 4):
                for l in range(j, 4):
                    dots[j][l] = dots[j][l] - mults[i][j] * dots[i][l]
                rows[j] = [rows[j][h] - mults[i][j] * rows[i][h] for h in range(2)]
            scaled.append([rows[i][h] * inv for h in range(2)])
        for i in (2, 1, 0):
            for j in range(i + 1, 4):
                scaled[i] = [scaled[i][h] - mults[i][j] * scaled[j][h] for h in range(2)]
        for g in range(g0 if r0 == 0 else g0 + 1, PANEL // 8):
            tile = groups[g]
            new = list(tile)
            for j in range(4):
                factor = spread_lane(tile[0], k + j)
                new = [new[h] - factor * scaled[j][h] for h in range(2)]
            if g == g0:
                new = [jnp.where(sub > 3, new[h], tile[h]) for h in range(2)]
            groups[g] = new
        for h in range(2):
            tile = groups[g0][h]
            for i in range(4):
                tile = jnp.where(sub == r0 + i, rows[i][h], tile)
            groups[g0] = [tile, groups[g0][1]] if h == 0 else [groups[g0][0], tile]


def exchange(a_ref, out_ref, feats, slices, partial, inbox, total, tall,
             rows, cols, pivot, owned, tz, ty, tq, tr, square,
             g1_s, g1_r, sib_s, sib_r, sl_s, sl_r, z_s, z_r, tz_s, tz_r, ty_s, ty_r, p1_s, p1_r,
             rows_s, rows_r, cols_s, cols_r, piv_s, piv_r, own_s, own_r, move_s, move_r):
    x, z, y, c = (lax.axis_index(name) for name in ("x", "z", "y", "c"))
    other = 1 - c
    mine = pl.ds(pl.multiple_of(x * SLICE, SLICE), SLICE)

    barrier = pltpu.get_barrier_semaphore()

    @pl.loop(1, NX * NY * NC)
    def _(i):
        there = (lax.rem(x + i // (NY * NC), NX), z, lax.rem(y + i // NC, NY), lax.rem(c + i, NC))
        pl.semaphore_signal(barrier, inc=1, device_id=there, device_id_type=MESH)

    @pl.loop(1, NZ)
    def _(d):
        there = (x, lax.rem(z + d, NZ), y, c)
        pl.semaphore_signal(barrier, inc=1, device_id=there, device_id_type=MESH)

    feats[c, x] = a_ref[...].T
    pl.semaphore_wait(barrier, NX * NY * NC - 1 + NZ - 1)
    for d in (1, 3, 2):
        send(feats.at[c, x], feats.at[c, x], g1_s.at[d], g1_r.at[x], (lax.rem(x + d, NX), z, y, c))

    def relay(piece):
        send(feats.at[c, piece], feats.at[c, piece], sib_s.at[piece], sib_r.at[piece], (x, z, y, other))
        for target in range(1, NY):
            @pl.when(target > y)
            def _():
                send(feats.at[c, piece, mine], slices.at[y, piece], sl_s.at[target, piece], sl_r.at[y, piece],
                     (x, z, target, c))
        slices[y, piece] = feats[c, piece, mine]

    relay(x)
    for d in (1, 3, 2):
        piece = lax.rem(x + d, NX)
        wait(feats.at[c, piece], g1_r.at[piece])
        relay(piece)
    for piece in range(NX):
        wait(feats.at[other, piece], sib_r.at[piece])

    def multiply(source):
        for half in range(NC):
            acc = jnp.zeros((SLICE, BLOCK), F32)
            for piece in range(NX):
                acc += lax.dot_general(slices[source, piece], feats[half, piece], (((1,), (1,)), ((), ())),
                                       preferred_element_type=F32)
            for s in range(SLICE // 8):
                partial[source, NC * s + half] = acc[8 * s:8 * s + 8]

    moved = {2: jnp.logical_or(y == 3, jnp.logical_and(y == 2, c == 0)), 3: jnp.logical_and(y == 3, c == 0)}
    taken = {2: jnp.logical_or(y == 0, jnp.logical_and(y == 1, c == 0)), 3: jnp.logical_and(y == 0, c == 0)}

    def owner_row(k):
        return jnp.where(taken[k], NY - 1 - y, y) if k in taken else y

    def active(k):
        own = k <= y
        return jnp.logical_or(jnp.logical_and(own, jnp.logical_not(moved[k])), taken[k]) if k in moved else own

    def halved(k):
        return jnp.logical_and(c == 1, y == k)

    def reduce_to_peers(k):
        @pl.when(jnp.logical_not(halved(k)))
        def _():
            @pl.loop(1, NZ)
            def _(d):
                target = lax.rem(z + d, NZ)
                send(partial.at[k, target], inbox.at[k, z], z_s.at[k], z_r.at[k], (x, target, y, c))
            pltpu.make_async_copy(partial.at[k, z], inbox.at[k, z], z_r.at[k]).start()

        @pl.when(halved(k))
        def _():
            @pl.loop(0, NZ // 2)
            def _(d):
                target = lax.rem(z + 2 * d + 1 - zc, NZ)

                @pl.when(target == z)
                def _():
                    pltpu.make_async_copy(partial.at[k, z], inbox.at[k, z], z_r.at[k]).start()

                @pl.when(target != z)
                def _():
                    send(partial.at[k, target], inbox.at[k, z], z_s.at[k], z_r.at[k], (x, target, y, c))

    def reduced(k):
        @pl.when(jnp.logical_and(active(k), jnp.logical_not(jnp.logical_and(halved(k), zc == 0))))
        def _():
            wait(inbox.at[k], z_r.at[k])
            total[k] = jnp.sum(inbox[k], axis=0)
            if k == 0:
                pl.when(jnp.logical_not(panel))(lambda: to_owner(k))
            else:
                to_owner(k)

    def sent_to_peers(k):
        @pl.when(active(k))
        def _():
            @pl.when(jnp.logical_not(halved(k)))
            def _():
                wait(partial.at[k, pl.ds(0, NZ - 1)], z_s.at[k])

            @pl.when(jnp.logical_and(halved(k), zc == 0))
            def _():
                wait(partial.at[k, pl.ds(0, NZ // 2)], z_s.at[k])

            @pl.when(jnp.logical_and(halved(k), zc == 1))
            def _():
                wait(partial.at[k, pl.ds(0, NZ // 2 - 1)], z_s.at[k])

    def taken_in(k):
        if k in taken:
            @pl.when(taken[k])
            def _():
                wait(partial.at[k], move_r.at[k])

    def arrived(source):
        @pl.when(source < y)
        def _():
            for piece in range(NX):
                wait(slices.at[source, piece], sl_r.at[source, piece])

    panel = jnp.logical_and(x < 2, c == 0)
    zs, zc = z // NC, lax.rem(z, NC)

    def to_owner(k):
        owner_z = 8 * c + 2 * x + zs // 4
        local = jnp.logical_and(jnp.logical_and(k == x, owner_z == z), jnp.logical_and(zc == c, owner_row(k) == y))
        slot = owned.at[lax.rem(zs, 4)]

        @pl.when(jnp.logical_not(local))
        def _():
            send(total.at[k], slot, own_s.at[k], own_r, (k, owner_z, owner_row(k), zc))

        @pl.when(local)
        def _():
            pltpu.make_async_copy(total.at[k], slot, own_r).start()

    def owner_sent(k):
        owner_z = 8 * c + 2 * x + zs // 4
        local = jnp.logical_and(jnp.logical_and(k == x, owner_z == z), jnp.logical_and(zc == c, owner_row(k) == y))
        sent = jnp.logical_and(active(k), jnp.logical_not(jnp.logical_and(halved(k), zc == 0)))

        @pl.when(jnp.logical_and(sent, jnp.logical_not(local)))
        def _():
            wait(total.at[k], own_s.at[k])

    arrived(0)
    multiply(0)
    reduce_to_peers(0)
    acc = jnp.zeros((8, 128), F32)
    for half in range(NC):
        for piece in range(NX):
            v = feats[half, piece].astype(F32)
            v = jnp.sum((v * v).reshape(BLOCK // 8, 8, BLOCK), axis=0)
            acc += v[:, :128] + v[:, 128:]
    tq[...] = acc

    @pl.loop(1, NZ)
    def _(d):
        target = lax.rem(z + d, NZ)
        send(tq, tz.at[z], tz_s, tz_r, (x, target, y, c))
    pltpu.make_async_copy(tq, tz.at[z], tz_r).start()

    for k in (2, 3, 1):
        @pl.when(k <= y)
        def _():
            arrived(k)
            multiply(k)
        if k in moved:
            @pl.when(moved[k])
            def _():
                send(partial.at[k], partial.at[k], move_s.at[k], move_r.at[k], (x, z, NY - 1 - y, c))
    pl.when(active(1))(lambda: reduce_to_peers(1))

    @pl.when(x >= 2)
    def _():
        for k in (2, 3):
            taken_in(k)
            pl.when(active(k))(lambda: reduce_to_peers(k))

    @pl.when(panel)
    def _():
        wait(inbox.at[0], z_r.at[0])
        total[0] = jnp.sum(inbox[0], axis=0)

        @pl.loop(1, NZ)
        def _(d):
            target = lax.rem(z + d, NZ)
            send(total.at[0], tall.at[zc, zs], p1_s, p1_r, (x, target, y, c))
        pltpu.make_async_copy(total.at[0], tall.at[zc, zs], p1_r).start()

    wait(tz, tz_r)
    tr[...] = jnp.sum(tz[...], axis=0)

    @pl.loop(1, NY)
    def _(d):
        send(tr, ty.at[y], ty_s, ty_r, (x, z, lax.rem(y + d, NY), c))
    pltpu.make_async_copy(tr, ty.at[y], ty_r).start()

    @pl.when(x < 2)
    def _():
        for k in (2, 3):
            taken_in(k)
            pl.when(active(k))(lambda: reduce_to_peers(k))

    pl.when(panel)(lambda: to_owner(0))
    pl.when(jnp.logical_not(panel))(lambda: reduced(0))

    col_half = z // 8
    col_lanes = pl.ds(pl.multiple_of(lax.rem(z, 8) // 4 * 128, 128), 128)

    def spread(src, dst, sems, recv, count, place):
        @pl.loop(0, count)
        def _(i):
            tx, ty_, tc = place(i)
            here = jnp.logical_and(jnp.logical_and(tx == x, ty_ == y), tc == c)

            @pl.when(here)
            def _():
                pltpu.make_async_copy(src, dst, recv).start()

            @pl.when(jnp.logical_not(here))
            def _():
                send(src, dst, sems.at[i], recv, (tx, z, ty_, tc))

    def spread_done(src, sems, count, place):
        @pl.loop(0, count)
        def _(i):
            tx, ty_, tc = place(i)
            here = jnp.logical_and(jnp.logical_and(tx == x, ty_ == y), tc == c)

            @pl.when(jnp.logical_not(here))
            def _():
                wait(src, sems.at[i])

    def place_pivot(i):
        return i // 8, lax.rem(i // 2, NY), lax.rem(i, NC)

    def place_cols(i):
        return y, i // 2, lax.rem(i, NC)

    def place_rows(half):
        return lambda i: (i, y, half)

    pivot_src = tall.at[0, :, :, pl.ds(0, 128)]
    cols_src = tall.at[col_half, :, :, col_lanes]

    @pl.when(panel)
    def _():
        wait(tall, p1_r)

        @pl.when(y == 0)
        def _():
            spread(pivot_src, pivot.at[x], piv_s, piv_r, 32, place_pivot)
        spread(cols_src, cols.at[x], cols_s, cols_r, 8, place_cols)
        for half in range(NC):
            spread(tall.at[half], rows.at[x], rows_s.at[half], rows_r, NX, place_rows(half))

    for k in range(1, NY):
        reduced(k)
    wait(pivot, piv_r)
    wait(ty, ty_r)
    damp = jnp.sum(jnp.sum(ty[...], axis=0), keepdims=True) * (SCALE * 0.01 / FULL)
    lane = lax.broadcasted_iota(jnp.int32, (8, PANEL), 1)
    sub = lax.broadcasted_iota(jnp.int32, (8, PANEL), 0)
    groups = []
    for g in range(PANEL // 8):
        diag = lane == sub + 8 * g
        left = pivot[g // 8, g % 8] * SCALE + jnp.where(diag, damp, 0.0)
        groups.append([left, jnp.where(diag, 1.0, 0.0).astype(F32)])
    eliminate(groups, 0, PANEL // 2, sub)
    for g in range(PANEL // 8):
        square[g, 0] = groups[g][0]
        square[g, 1] = groups[g][1]
    groups = [[square[g, 0], square[g, 1]] for g in range(PANEL // 8)]
    eliminate(groups, PANEL // 2, PANEL, sub)
    scaled = []
    for g in range(PANEL // 8):
        diag = jnp.sum(jnp.where(lane == sub + 8 * g, groups[g][0], 0.0), axis=1, keepdims=True)
        scaled.append(groups[g][1] * lax.rsqrt(diag))
    inverse = jnp.concatenate(scaled, axis=0)
    wait(cols, cols_r)
    wait(rows, rows_r)
    ids = lax.broadcasted_iota(jnp.int32, (PANEL, BLOCK), 0)
    row0 = (y * NC + c) * BLOCK
    row_ids = row0 + lax.broadcasted_iota(jnp.int32, (PANEL, BLOCK), 1)
    right = rows[...].reshape(PANEL, BLOCK) * SCALE + jnp.where(ids == row_ids, damp, 0.0)
    highest = lax.Precision.HIGHEST
    right = jnp.dot(inverse, right, precision=highest, preferred_element_type=F32)
    left = jnp.dot(inverse, cols[...].reshape(PANEL, PANEL) * SCALE, precision=highest, preferred_element_type=F32)
    update = lax.dot_general(left, right, (((0,), (0,)), ((), ())), precision=highest, preferred_element_type=F32)
    strip0 = (x * NZ + z) * 32
    leading = strip0 < PANEL
    picked = jnp.where(leading, right, update)
    wide = jnp.zeros((32, BLOCK), F32)
    for q in range(4):
        wide = jnp.where(lax.rem(z, 4) == q, picked[32 * q:32 * q + 32], wide)
    col_ids = strip0 + lax.broadcasted_iota(jnp.int32, (32, BLOCK), 0)
    row_ids = row0 + lax.broadcasted_iota(jnp.int32, (32, BLOCK), 1)

    @pl.when(NC * x + z // 8 <= NC * y + c)
    def _():
        wait(owned, own_r)
    schur = owned[...].reshape(32, BLOCK) * SCALE + jnp.where(col_ids == row_ids, damp, 0.0) - wide
    wide = jnp.where(leading, wide, schur)
    out_ref[...] = jnp.where(row_ids >= col_ids, wide, 0.0)

    for d in (1, 3, 2):
        wait(feats.at[c, x], g1_s.at[d])
    for piece in range(NX):
        wait(feats.at[c, piece], sib_s.at[piece])
        for target in range(1, NY):
            @pl.when(target > y)
            def _():
                wait(slices.at[y, piece], sl_s.at[target, piece])
    for k in range(NY):
        owner_sent(k)
        sent_to_peers(k)
    for k in moved:
        @pl.when(moved[k])
        def _():
            wait(partial.at[k], move_s.at[k])
    wait(tz.at[pl.ds(0, NZ - 1)], tz_s)
    wait(ty.at[pl.ds(0, NY - 1)], ty_s)

    @pl.when(panel)
    def _():
        for _ in range(1):
            wait(inbox.at[0, pl.ds(0, NZ - 1)], p1_s)

        @pl.when(y == 0)
        def _():
            spread_done(pivot_src, piv_s, 32, place_pivot)
        spread_done(cols_src, cols_s, 8, place_cols)
        for half in range(NC):
            spread_done(tall.at[half], rows_s.at[half], NX, place_rows(half))


def gathered(a):
    dma = pltpu.SemaphoreType.DMA
    vmem = pl.BlockSpec(memory_space=pltpu.VMEM)
    return pl.pallas_call(
        exchange,
        out_shape=jax.ShapeDtypeStruct((32, BLOCK), F32),
        in_specs=[vmem],
        out_specs=vmem,
        scratch_shapes=[
            pltpu.VMEM((NC, NX, BLOCK, BLOCK), BF16),
            pltpu.VMEM((NY, NX, SLICE, BLOCK), BF16),
            pltpu.VMEM((NY, NZ, 8, BLOCK), F32),
            pltpu.VMEM((NY, NZ, 8, BLOCK), F32),
            pltpu.VMEM((NY, 8, BLOCK), F32),
            pltpu.VMEM((NC, 8, 8, BLOCK), F32),
            pltpu.VMEM((2, 8, 8, BLOCK), F32),
            pltpu.VMEM((2, 8, 8, 128), F32),
            pltpu.VMEM((2, 8, 8, 128), F32),
            pltpu.VMEM((4, 8, BLOCK), F32),
            pltpu.VMEM((NZ, 8, 128), F32),
            pltpu.VMEM((NY, 8, 128), F32),
            pltpu.VMEM((8, 128), F32),
            pltpu.VMEM((8, 128), F32),
            pltpu.VMEM((PANEL // 8, 2, 8, PANEL), F32),
            dma((NX,)), dma((NX,)),
            dma((NX,)), dma((NX,)),
            dma((NY, NX)), dma((NY, NX)),
            dma((NY,)), dma((NY,)),
            dma(()), dma(()),
            dma(()), dma(()),
            dma(()), dma(()),
            dma((NC, NX)), dma(()),
            dma((8,)), dma(()),
            dma((32,)), dma(()),
            dma((NY,)), dma(()),
            dma((NY,)), dma((NY,)),
        ],
        compiler_params=pltpu.CompilerParams(collective_id=0, has_side_effects=True),
    )(a)


def shards(a):
    return gathered(a).T


def solution(mesh):
    finer = Mesh(mesh.devices.reshape(NX, NZ, NY, NC), ("x", "z", "y", "c"))
    return jax.shard_map(
        shards, mesh=finer, in_specs=(P(("x", "z"), ("y", "c")),), out_specs=P(("y", "c"), ("x", "z")), check_vma=False
    )
```

```python
import jax
import jax.numpy as jnp
from jax import lax
from jax.experimental import pallas as pl
from jax.experimental.pallas import tpu as pltpu
from jax.sharding import Mesh
from jax.sharding import PartitionSpec as P

MESH = pl.DeviceIdType.MESH
F32 = jnp.float32
BF16 = jnp.bfloat16
NX, NZ, NY, NC = 4, 16, 4, 2
BLOCK = 256
PANEL = 128
SLICE = BLOCK // NX
FULL = BLOCK * NY * NC
TOKENS = BLOCK * NX * NZ
SCALE = 2.0 / TOKENS


def far_first(i):
    return NZ // 2 + jnp.where(lax.rem(i, 2) == 0, i // 2, -((i + 1) // 2))


def wait(ref, sem):
    pltpu.make_async_copy(ref, ref, sem).wait()


def send(src, dst, send_sem, recv_sem, device):
    pltpu.make_async_remote_copy(
        src_ref=src,
        dst_ref=dst,
        send_sem=send_sem,
        recv_sem=recv_sem,
        device_id=device,
        device_id_type=MESH,
    ).start()


def spread_rows(row):
    return jnp.broadcast_to(row, (8, PANEL))


def spread_lane(tile, lane):
    return jnp.broadcast_to(tile[:, lane:lane + 1], (8, PANEL))


def eliminate(groups, first, last, sub):
    for k in range(first, last, 4):
        g0, r0 = k // 8, k % 8
        head = groups[g0]
        rows = [[spread_rows(head[h][r0 + i:r0 + i + 1]) for h in range(2)] for i in range(4)]
        dots = [[spread_lane(rows[i][0], k + j) if j >= i else None for j in range(4)] for i in range(4)]
        mults = [[None] * 4 for _ in range(4)]
        scaled = []
        for i in range(4):
            inv = 1.0 / dots[i][i]
            for j in range(i + 1, 4):
                mults[i][j] = dots[i][j] * inv
            for j in range(i + 1, 4):
                for l in range(j, 4):
                    dots[j][l] = dots[j][l] - mults[i][j] * dots[i][l]
                rows[j] = [rows[j][h] - mults[i][j] * rows[i][h] for h in range(2)]
            scaled.append([rows[i][h] * inv for h in range(2)])
        for i in (2, 1, 0):
            for j in range(i + 1, 4):
                scaled[i] = [scaled[i][h] - mults[i][j] * scaled[j][h] for h in range(2)]
        for g in range(g0 if r0 == 0 else g0 + 1, PANEL // 8):
            tile = groups[g]
            new = list(tile)
            for j in range(4):
                factor = spread_lane(tile[0], k + j)
                new = [new[h] - factor * scaled[j][h] for h in range(2)]
            if g == g0:
                new = [jnp.where(sub > 3, new[h], tile[h]) for h in range(2)]
            groups[g] = new
        for h in range(2):
            tile = groups[g0][h]
            for i in range(4):
                tile = jnp.where(sub == r0 + i, rows[i][h], tile)
            groups[g0] = [tile, groups[g0][1]] if h == 0 else [groups[g0][0], tile]


def exchange(a_ref, out_ref, feats, slices, partial, inbox, total, tall,
             rows, cols, pivot, owned, tz, ty, tq, tr, square, hubs, strip, many,
             g1_s, g1_r, sib_s, sib_r, sl_s, sl_r, z_s, z_r, tz_s, tz_r, ty_s, ty_r, p1_s, p1_r,
             rows_s, rows_r, cols_s, cols_r, piv_s, piv_r, own_s, own_r, move_s, move_r, hub_s, hub_r):
    x, z, y, c = (lax.axis_index(name) for name in ("x", "z", "y", "c"))
    other = 1 - c
    mine = pl.ds(pl.multiple_of(x * SLICE, SLICE), SLICE)

    barrier = pltpu.get_barrier_semaphore()

    @pl.loop(1, NX * NY * NC)
    def _(i):
        there = (lax.rem(x + i // (NY * NC), NX), z, lax.rem(y + i // NC, NY), lax.rem(c + i, NC))
        pl.semaphore_signal(barrier, inc=1, device_id=there, device_id_type=MESH)

    @pl.loop(1, NZ)
    def _(d):
        there = (x, lax.rem(z + d, NZ), y, c)
        pl.semaphore_signal(barrier, inc=1, device_id=there, device_id_type=MESH)

    feats[c, x] = a_ref[...].T
    pl.semaphore_wait(barrier, NX * NY * NC - 1 + NZ - 1)
    for d in (1, 3, 2):
        send(feats.at[c, x], feats.at[c, x], g1_s.at[d], g1_r.at[x], (lax.rem(x + d, NX), z, y, c))

    def relay(piece):
        send(feats.at[c, piece], feats.at[c, piece], sib_s.at[piece], sib_r.at[piece], (x, z, y, other))
        for target in range(1, NY):
            @pl.when(target > y)
            def _():
                send(feats.at[c, piece, mine], slices.at[y, piece], sl_s.at[target, piece], sl_r.at[y, piece],
                     (x, z, target, c))
        slices[y, piece] = feats[c, piece, mine]

    relay(x)
    for d in (1, 3, 2):
        piece = lax.rem(x + d, NX)
        wait(feats.at[c, piece], g1_r.at[piece])
        relay(piece)
    for piece in range(NX):
        wait(feats.at[other, piece], sib_r.at[piece])

    def multiply(source):
        for half in range(NC):
            acc = jnp.zeros((SLICE, BLOCK), F32)
            for piece in range(NX):
                acc += lax.dot_general(slices[source, piece], feats[half, piece], (((1,), (1,)), ((), ())),
                                       preferred_element_type=F32)
            for s in range(SLICE // 8):
                partial[source, NC * s + half] = acc[8 * s:8 * s + 8]

    moved = {2: jnp.logical_or(y == 3, jnp.logical_and(y == 2, c == 0)), 3: jnp.logical_and(y == 3, c == 0)}
    taken = {2: jnp.logical_or(y == 0, jnp.logical_and(y == 1, c == 0)), 3: jnp.logical_and(y == 0, c == 0)}

    def owner_row(k):
        return jnp.where(taken[k], NY - 1 - y, y) if k in taken else y

    def active(k):
        own = k <= y
        return jnp.logical_or(jnp.logical_and(own, jnp.logical_not(moved[k])), taken[k]) if k in moved else own

    def halved(k):
        return jnp.logical_and(c == 1, y == k)

    def reduce_to_peers(k):
        @pl.when(jnp.logical_not(halved(k)))
        def _():
            @pl.loop(0, NZ - 1)
            def _(d):
                target = lax.rem(z + far_first(d), NZ)
                send(partial.at[k, target], inbox.at[k, z], z_s.at[k], z_r.at[k], (x, target, y, c))
            pltpu.make_async_copy(partial.at[k, z], inbox.at[k, z], z_r.at[k]).start()

        @pl.when(halved(k))
        def _():
            @pl.loop(0, NZ // 2)
            def _(d):
                target = lax.rem(z + 2 * d + 1 - zc, NZ)

                @pl.when(target == z)
                def _():
                    pltpu.make_async_copy(partial.at[k, z], inbox.at[k, z], z_r.at[k]).start()

                @pl.when(target != z)
                def _():
                    send(partial.at[k, target], inbox.at[k, z], z_s.at[k], z_r.at[k], (x, target, y, c))

    def reduced(k):
        @pl.when(jnp.logical_and(active(k), jnp.logical_not(jnp.logical_and(halved(k), zc == 0))))
        def _():
            wait(inbox.at[k], z_r.at[k])
            total[k] = jnp.sum(inbox[k], axis=0)
            if k == 0:
                pl.when(jnp.logical_not(panel))(lambda: to_owner(k))
            else:
                to_owner(k)

    def sent_to_peers(k):
        @pl.when(active(k))
        def _():
            @pl.when(jnp.logical_not(halved(k)))
            def _():
                wait(partial.at[k, pl.ds(0, NZ - 1)], z_s.at[k])

            @pl.when(jnp.logical_and(halved(k), zc == 0))
            def _():
                wait(partial.at[k, pl.ds(0, NZ // 2)], z_s.at[k])

            @pl.when(jnp.logical_and(halved(k), zc == 1))
            def _():
                wait(partial.at[k, pl.ds(0, NZ // 2 - 1)], z_s.at[k])

    def taken_in(k):
        if k in taken:
            @pl.when(taken[k])
            def _():
                wait(partial.at[k], move_r.at[k])

    def arrived(source):
        @pl.when(source < y)
        def _():
            for piece in range(NX):
                wait(slices.at[source, piece], sl_r.at[source, piece])

    panel = jnp.logical_and(x < 2, c == 0)
    zs, zc = z // NC, lax.rem(z, NC)

    def to_owner(k):
        owner_z = 8 * c + 2 * x + zs // 4
        local = jnp.logical_and(jnp.logical_and(k == x, owner_z == z), jnp.logical_and(zc == c, owner_row(k) == y))
        slot = owned.at[lax.rem(zs, 4)]

        @pl.when(jnp.logical_not(local))
        def _():
            send(total.at[k], slot, own_s.at[k], own_r, (k, owner_z, owner_row(k), zc))

        @pl.when(local)
        def _():
            pltpu.make_async_copy(total.at[k], slot, own_r).start()

    def owner_sent(k):
        owner_z = 8 * c + 2 * x + zs // 4
        local = jnp.logical_and(jnp.logical_and(k == x, owner_z == z), jnp.logical_and(zc == c, owner_row(k) == y))
        sent = jnp.logical_and(active(k), jnp.logical_not(jnp.logical_and(halved(k), zc == 0)))

        @pl.when(jnp.logical_and(sent, jnp.logical_not(local)))
        def _():
            wait(total.at[k], own_s.at[k])

    arrived(0)
    multiply(0)
    reduce_to_peers(0)
    tracer = jnp.logical_and(x == NX - 1, c == 1)

    @pl.when(tracer)
    def _():
        acc = jnp.zeros((8, 128), F32)
        for half in range(NC):
            for piece in range(NX):
                v = feats[half, piece].astype(F32)
                v = jnp.sum((v * v).reshape(BLOCK // 8, 8, BLOCK), axis=0)
                acc += v[:, :128] + v[:, 128:]
        tq[...] = acc

        @pl.loop(0, NZ - 1)
        def _(d):
            target = lax.rem(z + far_first(d), NZ)
            send(tq, tz.at[z], tz_s, tz_r, (x, target, y, c))
        pltpu.make_async_copy(tq, tz.at[z], tz_r).start()

    for k in (2, 3, 1):
        @pl.when(k <= y)
        def _():
            arrived(k)
            multiply(k)
        if k in moved:
            @pl.when(moved[k])
            def _():
                send(partial.at[k], partial.at[k], move_s.at[k], move_r.at[k], (x, z, NY - 1 - y, c))
    pl.when(jnp.logical_and(active(1), jnp.logical_not(panel)))(lambda: reduce_to_peers(1))

    @pl.when(x >= 2)
    def _():
        for k in (2, 3):
            taken_in(k)
            pl.when(active(k))(lambda: reduce_to_peers(k))

    pl.when(jnp.logical_not(panel))(lambda: reduced(0))
    piv_chunk = total.at[0, :, pl.ds(0, 128)]
    hub = jnp.logical_and(y == 0, c == 0)

    @pl.when(panel)
    def _():
        wait(inbox.at[0], z_r.at[0])
        total[0] = jnp.sum(inbox[0], axis=0)

        @pl.when(jnp.logical_and(y == 0, zc == 0))
        def _():
            @pl.loop(0, NX * NZ)
            def _(i):
                tx = lax.rem(x + i // NZ, NX)
                tz_ = lax.rem(z + NZ // 2 + i, NZ)
                here = jnp.logical_and(tx == x, tz_ == z)

                @pl.when(here)
                def _():
                    pltpu.make_async_copy(piv_chunk, hubs.at[x, zs], hub_r).start()

                @pl.when(jnp.logical_not(here))
                def _():
                    send(piv_chunk, hubs.at[x, zs], hub_s, hub_r, (tx, tz_, y, c))

        @pl.loop(0, NZ - 1)
        def _(d):
            target = lax.rem(z + far_first(d), NZ)
            send(total.at[0], tall.at[zc, zs], p1_s, p1_r, (x, target, y, c))
        pltpu.make_async_copy(total.at[0], tall.at[zc, zs], p1_r).start()
        pl.when(active(1))(lambda: reduce_to_peers(1))

    @pl.when(x < 2)
    def _():
        for k in (2, 3):
            taken_in(k)
            pl.when(active(k))(lambda: reduce_to_peers(k))

    pl.when(panel)(lambda: to_owner(0))

    @pl.when(tracer)
    def _():
        wait(tz, tz_r)
        tr[...] = jnp.sum(tz[...], axis=0)

        @pl.loop(1, NX * NY * NC)
        def _(i):
            there = (lax.rem(x + i // (NY * NC), NX), z, lax.rem(y + i // NC, NY), lax.rem(c + i, NC))
            send(tr, ty.at[y], ty_s, ty_r, there)
        pltpu.make_async_copy(tr, ty.at[y], ty_r).start()

    @pl.when(hub)
    def _():
        wait(hubs, hub_r)

        @pl.loop(1, NY * NC)
        def _(i):
            send(hubs, pivot, piv_s.at[i], piv_r, (x, z, lax.rem(y + i // NC, NY), lax.rem(c + i, NC)))
        pltpu.make_async_copy(hubs, pivot, piv_r).start()

    def spread(src, dst, sems, recv, count, place):
        @pl.loop(0, count)
        def _(i):
            tx, ty_, tc = place(i)
            here = jnp.logical_and(jnp.logical_and(tx == x, ty_ == y), tc == c)

            @pl.when(here)
            def _():
                pltpu.make_async_copy(src, dst, recv).start()

            @pl.when(jnp.logical_not(here))
            def _():
                send(src, dst, sems.at[i], recv, (tx, z, ty_, tc))

    def spread_done(src, sems, count, place):
        @pl.loop(0, count)
        def _(i):
            tx, ty_, tc = place(i)
            here = jnp.logical_and(jnp.logical_and(tx == x, ty_ == y), tc == c)

            @pl.when(jnp.logical_not(here))
            def _():
                wait(src, sems.at[i])

    def place_cols(i):
        return y, i // 2, lax.rem(i, NC)

    def place_rows(half):
        return lambda i: (i, y, half)

    @pl.when(panel)
    def _():
        wait(tall, p1_r)
        mixed = tall[z // 8].reshape(SLICE, BLOCK)
        mixed = jnp.where(lax.rem(z, 8) >= 4, mixed[:, 128:], mixed[:, :128])
        lanes = lax.broadcasted_iota(jnp.int32, (16, 128), 1) // 32
        packed = jnp.zeros((16, 128), F32)
        for q in range(4):
            turned = pltpu.roll(mixed[16 * q:16 * q + 16], lax.rem(32 * q - 32 * lax.rem(z, 4) + 128, 128), 1)
            packed = jnp.where(lanes == q, turned, packed)
        strip[...] = packed
        for half in range(NC):
            spread(tall.at[half], rows.at[x], rows_s.at[half], rows_r, NX, place_rows(half))
        spread(strip, cols.at[x], cols_s, cols_r, 8, place_cols)

    wait(pivot, piv_r)
    wait(ty, ty_r)
    damp = jnp.sum(jnp.sum(ty[...], axis=0), keepdims=True) * (SCALE * 0.01 / FULL)
    lane = lax.broadcasted_iota(jnp.int32, (8, PANEL), 1)
    sub = lax.broadcasted_iota(jnp.int32, (8, PANEL), 0)
    groups = []
    for g in range(PANEL // 8):
        diag = lane == sub + 8 * g
        left = pivot[g // 8, g % 8] * SCALE + jnp.where(diag, damp, 0.0)
        groups.append([left, jnp.where(diag, 1.0, 0.0).astype(F32)])
    eliminate(groups, 0, PANEL // 2, sub)
    for g in range(PANEL // 8):
        square[g, 0] = groups[g][0]
        square[g, 1] = groups[g][1]
    for k in range(1, NY):
        reduced(k)
    groups = [[square[g, 0], square[g, 1]] for g in range(PANEL // 8)]
    eliminate(groups, PANEL // 2, PANEL, sub)
    scaled = []
    for g in range(PANEL // 8):
        diag = jnp.sum(jnp.where(lane == sub + 8 * g, groups[g][0], 0.0), axis=1, keepdims=True)
        scaled.append(groups[g][1] * lax.rsqrt(diag))
    inverse = jnp.concatenate(scaled, axis=0)
    wait(cols, cols_r)
    wait(rows, rows_r)
    ids = lax.broadcasted_iota(jnp.int32, (PANEL, BLOCK), 0)
    row0 = (y * NC + c) * BLOCK
    row_ids = row0 + lax.broadcasted_iota(jnp.int32, (PANEL, BLOCK), 1)
    right = rows[...].reshape(PANEL, BLOCK) * SCALE + jnp.where(ids == row_ids, damp, 0.0)
    highest = lax.Precision.HIGHEST
    right = jnp.dot(inverse, right, precision=highest, preferred_element_type=F32)
    left = jnp.concatenate([pltpu.roll(cols[h], (128 - 32 * q) % 128, 1) for h in range(2) for q in range(4)], axis=0)
    left = jnp.dot(inverse, left * SCALE, precision=highest, preferred_element_type=F32)
    update = lax.dot_general(left, right, (((0,), (0,)), ((), ())), precision=highest, preferred_element_type=F32)
    strip0 = (x * NZ + z) * 32
    leading = strip0 < PANEL
    wide = update[:32]
    for q in range(4):
        wide = jnp.where(jnp.logical_and(leading, z == q), right[32 * q:32 * q + 32], wide)
    col_ids = strip0 + lax.broadcasted_iota(jnp.int32, (32, BLOCK), 0)
    row_ids = row0 + lax.broadcasted_iota(jnp.int32, (32, BLOCK), 1)

    @pl.when(NC * x + z // 8 <= NC * y + c)
    def _():
        wait(owned, own_r)
    schur = owned[...].reshape(32, BLOCK) * SCALE + jnp.where(col_ids == row_ids, damp, 0.0) - wide
    wide = jnp.where(leading, wide, schur)
    out_ref[...] = jnp.where(row_ids >= col_ids, wide, 0.0)

    for d in (1, 3, 2):
        wait(feats.at[c, x], g1_s.at[d])
    for piece in range(NX):
        wait(feats.at[c, piece], sib_s.at[piece])
        for target in range(1, NY):
            @pl.when(target > y)
            def _():
                wait(slices.at[y, piece], sl_s.at[target, piece])
    for k in range(NY):
        owner_sent(k)
        sent_to_peers(k)
    for k in moved:
        @pl.when(moved[k])
        def _():
            wait(partial.at[k], move_s.at[k])
    @pl.when(tracer)
    def _():
        wait(tz.at[pl.ds(0, NZ - 1)], tz_s)
        wait(many.at[pl.ds(0, NX * NY * NC - 1)], ty_s)

    @pl.when(hub)
    def _():
        @pl.loop(1, NY * NC)
        def _(i):
            wait(hubs, piv_s.at[i])

    @pl.when(panel)
    def _():
        wait(inbox.at[0, pl.ds(0, NZ - 1)], p1_s)

        @pl.when(jnp.logical_and(y == 0, zc == 0))
        def _():
            wait(many.at[pl.ds(0, NX * NZ - 1)], hub_s)
        spread_done(strip, cols_s, 8, place_cols)
        for half in range(NC):
            spread_done(tall.at[half], rows_s.at[half], NX, place_rows(half))


def gathered(a):
    dma = pltpu.SemaphoreType.DMA
    vmem = pl.BlockSpec(memory_space=pltpu.VMEM)
    return pl.pallas_call(
        exchange,
        out_shape=jax.ShapeDtypeStruct((32, BLOCK), F32),
        in_specs=[vmem],
        out_specs=vmem,
        scratch_shapes=[
            pltpu.VMEM((NC, NX, BLOCK, BLOCK), BF16),
            pltpu.VMEM((NY, NX, SLICE, BLOCK), BF16),
            pltpu.VMEM((NY, NZ, 8, BLOCK), F32),
            pltpu.VMEM((NY, NZ, 8, BLOCK), F32),
            pltpu.VMEM((NY, 8, BLOCK), F32),
            pltpu.VMEM((NC, 8, 8, BLOCK), F32),
            pltpu.VMEM((2, 8, 8, BLOCK), F32),
            pltpu.VMEM((2, 16, 128), F32),
            pltpu.VMEM((2, 8, 8, 128), F32),
            pltpu.VMEM((4, 8, BLOCK), F32),
            pltpu.VMEM((NZ, 8, 128), F32),
            pltpu.VMEM((NY, 8, 128), F32),
            pltpu.VMEM((8, 128), F32),
            pltpu.VMEM((8, 128), F32),
            pltpu.VMEM((PANEL // 8, 2, 8, PANEL), F32),
            pltpu.VMEM((2, 8, 8, 128), F32),
            pltpu.VMEM((16, 128), F32),
            pltpu.VMEM((64, 8, 128), F32),
            dma((NX,)), dma((NX,)),
            dma((NX,)), dma((NX,)),
            dma((NY, NX)), dma((NY, NX)),
            dma((NY,)), dma((NY,)),
            dma(()), dma(()),
            dma(()), dma(()),
            dma(()), dma(()),
            dma((NC, NX)), dma(()),
            dma((8,)), dma(()),
            dma((8,)), dma(()),
            dma((NY,)), dma(()),
            dma((NY,)), dma((NY,)),
            dma(()), dma(()),
        ],
        compiler_params=pltpu.CompilerParams(collective_id=0, has_side_effects=True),
    )(a)


def shards(a):
    return gathered(a).T


def solution(mesh):
    finer = Mesh(mesh.devices.reshape(NX, NZ, NY, NC), ("x", "z", "y", "c"))
    return jax.shard_map(
        shards, mesh=finer, in_specs=(P(("x", "z"), ("y", "c")),), out_specs=P(("y", "c"), ("x", "z")), check_vma=False
    )
```

```python
import jax
import jax.numpy as jnp
from jax import lax
from jax.experimental import pallas as pl
from jax.experimental.pallas import tpu as pltpu
from jax.sharding import Mesh
from jax.sharding import PartitionSpec as P

MESH = pl.DeviceIdType.MESH
F32 = jnp.float32
BF16 = jnp.bfloat16
NX, NZ, NY, NC = 4, 16, 4, 2
BLOCK = 256
PANEL = 128
SLICE = BLOCK // NX
STRIPS = 8
FULL = BLOCK * NY * NC
TOKENS = BLOCK * NX * NZ
SCALE = 2.0 / TOKENS
PLANE = NX * NY * NC
GATES = 1


def wait(ref, sem):
    pltpu.make_async_copy(ref, ref, sem).wait()


def local(src, dst, sem):
    pltpu.make_async_copy(src, dst, sem).start()


def send(src, dst, send_sem, recv_sem, device):
    pltpu.make_async_remote_copy(
        src_ref=src,
        dst_ref=dst,
        send_sem=send_sem,
        recv_sem=recv_sem,
        device_id=device,
        device_id_type=MESH,
    ).start()


def far_first(i):
    return NZ // 2 + jnp.where(lax.rem(i, 2) == 0, i // 2, -((i + 1) // 2))


def both(*conditions):
    out = conditions[0]
    for condition in conditions[1:]:
        out = jnp.logical_and(out, condition)
    return out


def neither(condition):
    return jnp.logical_not(condition)


def spread_rows(row):
    return jnp.broadcast_to(row, (8, PANEL))


def spread_lane(tile, lane):
    return jnp.broadcast_to(tile[:, lane:lane + 1], (8, PANEL))


def eliminate(groups, first, last, sub):
    for k in range(first, last, 4):
        g0, r0 = k // 8, k % 8
        head = groups[g0]
        rows = [[spread_rows(head[h][r0 + i:r0 + i + 1]) for h in range(2)] for i in range(4)]
        dots = [[spread_lane(rows[i][0], k + j) if j >= i else None for j in range(4)] for i in range(4)]
        mults = [[None] * 4 for _ in range(4)]
        scaled = []
        for i in range(4):
            inv = 1.0 / dots[i][i]
            for j in range(i + 1, 4):
                mults[i][j] = dots[i][j] * inv
            for j in range(i + 1, 4):
                for l in range(j, 4):
                    dots[j][l] = dots[j][l] - mults[i][j] * dots[i][l]
                rows[j] = [rows[j][h] - mults[i][j] * rows[i][h] for h in range(2)]
            scaled.append([rows[i][h] * inv for h in range(2)])
        for i in (2, 1, 0):
            for j in range(i + 1, 4):
                scaled[i] = [scaled[i][h] - mults[i][j] * scaled[j][h] for h in range(2)]
        for g in range(g0 if r0 == 0 else g0 + 1, PANEL // 8):
            tile = groups[g]
            new = list(tile)
            for j in range(4):
                factor = spread_lane(tile[0], k + j)
                new = [new[h] - factor * scaled[j][h] for h in range(2)]
            if g == g0:
                new = [jnp.where(sub > 3, new[h], tile[h]) for h in range(2)]
            groups[g] = new
        for h in range(2):
            tile = groups[g0][h]
            for i in range(4):
                tile = jnp.where(sub == r0 + i, rows[i][h], tile)
            groups[g0] = [tile, groups[g0][1]] if h == 0 else [groups[g0][0], tile]


def exchange(a_ref, out_ref, feats, slices, partial, inbox, total, pin, psum, tall, rows, cols, pivot, owned,
             tz, ty, tq, tr, square, hubs, strip, many, gram, gin, gpart, gx, gtot,
             g1_s, g1_r, sib_s, sib_r, sl_s, sl_r, z_s, z_r, tz_s, tz_r, ty_s, ty_r, p0_s, p0_r, p1_s, p1_r,
             rows_s, rows_r, cols_s, cols_r, piv_s, piv_r, own_s, own_r, move_s, move_r, hub_s, hub_r, gz_s, gz_r, gx_s, gx_r, gate):
    x, z, y, c = (lax.axis_index(name) for name in ("x", "z", "y", "c"))
    other = 1 - c

    def along(d):
        return (x, lax.rem(z + d + NZ, NZ), y, c)

    def in_plane(i):
        return (lax.rem(x + i // (NY * NC), NX), z, lax.rem(y + i // NC, NY), lax.rem(c + i, NC))

    barrier = pltpu.get_barrier_semaphore()

    @pl.loop(1, PLANE)
    def _(i):
        pl.semaphore_signal(barrier, inc=1, device_id=in_plane(i), device_id_type=MESH)

    @pl.loop(1, NZ)
    def _(d):
        pl.semaphore_signal(barrier, inc=1, device_id=along(d), device_id_type=MESH)

    feats[c, x] = a_ref[...].T
    pl.semaphore_wait(barrier, PLANE - 1 + NZ - 1)
    hub = both(y == 0, c == 0)
    panel = c == 0
    place = lax.rem(z + 4, NZ)
    holder = both(panel, place < STRIPS)
    place_s, place_h = place // NC, lax.rem(place, NC)

    def part(piece, h):
        return feats.at[c, piece, pl.ds(128 * h, 128)]

    def pass_on(piece, h, step, sem):
        send(part(piece, h), part(piece, h), g1_s.at[sem], g1_r.at[piece, h], (lax.rem(x + step, NX), z, y, c))

    def relay(piece, h):
        send(part(piece, h), part(piece, h), sib_s.at[piece], sib_r.at[piece], (x, z, y, other))
        parts = []
        for k in range(4 * h, 4 * h + 4):
            start = pl.multiple_of(32 * k + 16 * (x // 2), 16)
            tile = feats[c, piece, pl.ds(start, 16)].astype(F32)
            parts.append(jnp.where(lax.rem(x, 2) == 1, tile[8:], tile[:8]))
        slices[y, piece, pl.ds(32 * h, 32)] = jnp.concatenate(parts, axis=0).astype(BF16)
        for target in range(1, NY):
            @pl.when(target > y)
            def _():
                there = slices.at[y, piece, pl.ds(32 * h, 32)]
                send(there, there, sl_s.at[target, piece], sl_r.at[y, piece], (x, z, target, c))

    pass_on(x, 0, 1, 0)
    pass_on(x, 1, 3, 1)
    pass_on(x, 1, 1, 2)
    pass_on(x, 0, 3, 3)
    relay(x, 0)
    relay(x, 1)

    def gram_out():
        block = feats[c, x, :PANEL]
        block = lax.dot_general(block, block, (((1,), (1,)), ((), ())), preferred_element_type=F32)
        gram[...] = block.reshape(STRIPS, 16, PANEL)
        for n in range(STRIPS):
            target = (12 + n) % NZ
            pl.when(target == z)(lambda: local(gram.at[n], gin.at[z], gz_r))
            pl.when(target != z)(lambda: send(gram.at[n], gin.at[z], gz_s, gz_r, (x, target, y, c)))

    left_x, right_x, far_x = lax.rem(x + 3, NX), lax.rem(x + 1, NX), lax.rem(x + 2, NX)
    for i, (piece, h, step) in enumerate(
        ((left_x, 0, 1), (right_x, 1, 3), (left_x, 1, 0), (right_x, 0, 0), (far_x, 0, 0), (far_x, 1, 0))
    ):
        wait(part(piece, h), g1_r.at[piece, h])
        if step:
            pass_on(piece, h, step, 4 + h)
        relay(piece, h)
        if i == 0:
            pl.when(hub)(gram_out)

    @pl.when(both(hub, holder))
    def _():
        wait(gin, gz_r)
        gpart[...] = jnp.sum(gin[...], axis=0)
        for d in (1, 3, 2):
            send(gpart, gx.at[x], gx_s.at[d], gx_r, (lax.rem(x + d, NX), z, y, c))
        local(gpart, gx.at[x], gx_r)
    for piece in range(NX):
        wait(feats.at[other, piece], sib_r.at[piece])

    moved = {2: y == 3}
    taken = {2: y == 0}
    gets = z // STRIPS == c

    def owner_row(k):
        return jnp.where(taken[k], NY - 1 - y, y) if k in taken else y

    def active(k):
        own = k <= y
        return jnp.logical_or(both(own, neither(moved[k])), taken[k]) if k in moved else own

    def halved(k):
        return both(c == 1, y == k)

    def first_strip(k):
        return jnp.where(panel, 4, 0) if k == 0 else 0

    def receives(k):
        return both(gets, active(k), lax.rem(z, STRIPS) >= first_strip(k))

    def arrived(source):
        @pl.when(source < y)
        def _():
            for piece in range(NX):
                wait(slices.at[source, piece], sl_r.at[source, piece])

    def multiply(source):
        for half in range(NC):
            acc = jnp.zeros((SLICE, BLOCK), F32)
            for piece in range(NX):
                acc += lax.dot_general(slices[source, piece], feats[half, piece], (((1,), (1,)), ((), ())),
                                       preferred_element_type=F32)
            for s in range(STRIPS):
                partial[source, s, half] = acc[8 * s:8 * s + 8]

    def reduce_to_peers(ks, when):
        @pl.loop(0, NZ)
        def _(i):
            target = lax.rem(z + jnp.where(i == NZ - 1, 0, far_first(i)), NZ)
            s = lax.rem(target, STRIPS)
            for k in ks:
                src, dst = partial.at[k, s], inbox.at[k, z]
                fits = both(when(k), target // STRIPS == c, s >= first_strip(k))

                def go(src, dst):
                    pl.when(target == z)(lambda: local(src, dst, z_r.at[k]))
                    pl.when(target != z)(lambda: send(src, dst, z_s.at[k], z_r.at[k], (x, target, y, c)))

                pl.when(both(fits, neither(halved(k))))(lambda: go(src, dst))
                pl.when(both(fits, halved(k)))(lambda: go(src.at[1], dst.at[1]))

    def sent_to_peers(k):
        count = STRIPS - first_strip(k) - jnp.where(receives(k), 1, 0)
        for n in (3, 4, 7, 8):
            if n < 5 and k > 0:
                continue

            @pl.when(both(active(k), count == n, neither(halved(k))))
            def _():
                wait(partial.at[k, pl.ds(0, n)], z_s.at[k])

            @pl.when(both(active(k), count == n, halved(k)))
            def _():
                wait(partial.at[k, pl.ds(0, n), 1], z_s.at[k])

    def owners(k, act):
        for half in range(NC):
            needed = receives(k) if half == 1 else both(receives(k), neither(halved(k)))
            here = both(k == x, owner_row(k) == y, half == c)

            if act == "start":
                pl.when(both(needed, here))(lambda: local(total.at[k, half], owned.at[x], own_r))

            @pl.when(both(needed, neither(here)))
            def _():
                if act == "start":
                    send(total.at[k, half], owned.at[x], own_s.at[k, half], own_r, (k, z, owner_row(k), half))
                else:
                    wait(total.at[k, half], own_s.at[k, half])

    def reduced(k):
        @pl.when(both(receives(k), neither(halved(k))))
        def _():
            wait(inbox.at[k], z_r.at[k])
            total[k] = jnp.sum(inbox[k], axis=0)

        @pl.when(both(receives(k), halved(k)))
        def _():
            wait(inbox.at[k, :, 1], z_r.at[k])
            total[k, 1] = jnp.sum(inbox[k, :, 1], axis=0)
        owners(k, "start")

    def taken_in(k):
        if k in taken:
            @pl.when(taken[k])
            def _():
                wait(partial.at[k], move_r.at[k])

    arrived(0)
    multiply(0)

    @pl.when(panel)
    def _():
        for n in range(STRIPS):
            target = (12 + n) % NZ

            @pl.when(target == z)
            def _():
                local(partial.at[0, n // NC, n % NC], pin.at[z], p0_r)

            @pl.when(target != z)
            def _():
                send(partial.at[0, n // NC, n % NC], pin.at[z], p0_s, p0_r, (x, target, y, c))

    @pl.when(both(hub, holder))
    def _():
        wait(gx, gx_r)
        gtot[...] = jnp.sum(gx[...], axis=0)

        @pl.loop(0, NZ - 1)
        def _(d):
            send(gtot, hubs.at[place], hub_s, hub_r, along(far_first(d)))
        local(gtot, hubs.at[place], hub_r)

    tracer = both(x == NX - 1, c == 1)

    @pl.when(tracer)
    def _():
        acc = jnp.zeros((8, 128), F32)
        for half in range(NC):
            for piece in range(NX):
                v = feats[half, piece].astype(F32)
                v = jnp.sum((v * v).reshape(BLOCK // 8, 8, BLOCK), axis=0)
                acc += v[:, :128] + v[:, 128:]
        tq[...] = acc

        @pl.loop(0, NZ - 1)
        def _(d):
            send(tq, tz.at[z], tz_s, tz_r, along(far_first(d)))
        local(tq, tz.at[z], tz_r)

    for k in (2, 3, 1):
        @pl.when(k <= y)
        def _():
            arrived(k)
            multiply(k)
        if k in moved:
            @pl.when(moved[k])
            def _():
                send(partial.at[k], partial.at[k], move_s.at[k], move_r.at[k], (x, z, NY - 1 - y, c))

    def kept(k):
        return both(active(k), neither(taken[k])) if k in taken else active(k)

    pl.when(panel)(lambda: reduce_to_peers((0, 1), kept))

    @pl.when(holder)
    def _():
        wait(pin, p0_r)
        psum[...] = jnp.sum(pin[...], axis=0)

        @pl.loop(0, NZ - 1)
        def _(d):
            send(psum, tall.at[place_h, place_s], p1_s, p1_r, along(far_first(d)))
        local(psum, tall.at[place_h, place_s], p1_r)

    pl.when(panel)(lambda: reduce_to_peers((2, 3), kept))

    @pl.when(neither(panel))
    def _():
        for n in range(GATES):
            pl.semaphore_signal(gate.at[n], inc=1, device_id=along(8), device_id_type=MESH)
            pl.semaphore_wait(gate.at[n], 1)
        reduce_to_peers((0, 1, 2, 3), kept)

    taken_in(2)
    pl.when(taken[2])(lambda: reduce_to_peers((2,), active))

    @pl.when(tracer)
    def _():
        wait(tz, tz_r)
        tr[...] = jnp.sum(tz[...], axis=0)

        @pl.loop(1, PLANE)
        def _(i):
            send(tr, ty.at[y], ty_s, ty_r, in_plane(i))
        local(tr, ty.at[y], ty_r)

    @pl.when(hub)
    def _():
        wait(hubs, hub_r)

        @pl.loop(1, NY * NC)
        def _(i):
            send(hubs, pivot, piv_s.at[i], piv_r, (x, z, lax.rem(y + i // NC, NY), lax.rem(c + i, NC)))
        local(hubs, pivot, piv_r)

    def spread(src, dst, sems, recv, count, where, start):
        @pl.loop(0, count)
        def _(i):
            tx, to_y, tc = where(i)
            here = both(tx == x, to_y == y, tc == c)
            if start:
                pl.when(here)(lambda: local(src, dst, recv))
                pl.when(neither(here))(lambda: send(src, dst, sems.at[i], recv, (tx, z, to_y, tc)))
            else:
                pl.when(neither(here))(lambda: wait(src, sems.at[i]))

    def spread_panel(start):
        for half in range(NC):
            spread(tall.at[half], rows.at[x], rows_s.at[half], rows_r, NX, lambda i: (lax.rem(x + i, NX), y, half), start)
        spread(strip, cols.at[x], cols_s, cols_r, NY * NC, lambda i: (y, i // 2, lax.rem(i, NC)), start)

    @pl.when(panel)
    def _():
        wait(tall, p1_r)
        mixed = tall[z // 8].reshape(32, BLOCK)
        mixed = jnp.where(lax.rem(z, 8) >= 4, mixed[:, 128:], mixed[:, :128])
        lanes = lax.broadcasted_iota(jnp.int32, (8, 128), 1) // 32
        packed = jnp.zeros((8, 128), F32)
        for q in range(4):
            turned = pltpu.roll(mixed[8 * q:8 * q + 8], lax.rem(32 * q - 32 * lax.rem(z, 4) + 128, 128), 1)
            packed = jnp.where(lanes == q, turned, packed)
        strip[...] = packed
        spread_panel(True)

    wait(pivot, piv_r)
    wait(ty, ty_r)
    damp = jnp.sum(jnp.sum(ty[...], axis=0), keepdims=True) * (SCALE * 0.01 / FULL)
    lane = lax.broadcasted_iota(jnp.int32, (8, PANEL), 1)
    sub = lax.broadcasted_iota(jnp.int32, (8, PANEL), 0)
    groups = []
    for g in range(PANEL // 8):
        diag = lane == sub + 8 * g
        left = pivot[g // 2, 8 * (g % 2):8 * (g % 2) + 8] * SCALE + jnp.where(diag, damp, 0.0)
        groups.append([left, jnp.where(diag, 1.0, 0.0).astype(F32)])
    eliminate(groups, 0, PANEL // 2, sub)
    for g in range(PANEL // 8):
        square[g, 0] = groups[g][0]
        square[g, 1] = groups[g][1]
    for k in range(NY):
        reduced(k)
    groups = [[square[g, 0], square[g, 1]] for g in range(PANEL // 8)]
    eliminate(groups, PANEL // 2, PANEL, sub)
    scaled = []
    for g in range(PANEL // 8):
        diag = jnp.sum(jnp.where(lane == sub + 8 * g, groups[g][0], 0.0), axis=1, keepdims=True)
        scaled.append(groups[g][1] * lax.rsqrt(diag))
    inverse = jnp.concatenate(scaled, axis=0)
    wait(cols, cols_r)
    wait(rows, rows_r)
    ids = lax.broadcasted_iota(jnp.int32, (PANEL, BLOCK), 0)
    row0 = (y * NC + c) * BLOCK
    row_ids = row0 + lax.broadcasted_iota(jnp.int32, (PANEL, BLOCK), 1)
    right = jnp.concatenate([rows[i, q] for q in range(4) for i in range(NX)], axis=0)
    right = right * SCALE + jnp.where(ids == row_ids, damp, 0.0)
    highest = lax.Precision.HIGHEST
    right = jnp.dot(inverse, right, precision=highest, preferred_element_type=F32)
    left = jnp.concatenate([pltpu.roll(cols[i], (128 - 32 * q) % 128, 1) for q in range(4) for i in range(NX)], axis=0)
    left = jnp.dot(inverse, left * SCALE, precision=highest, preferred_element_type=F32)
    update = lax.dot_general(left, right, (((0,), (0,)), ((), ())), precision=highest, preferred_element_type=F32)
    strip0 = (x * NZ + z) * 32
    leading = strip0 < PANEL
    wide = update[:32]
    for q in range(4):
        wide = jnp.where(both(leading, z == q), right[32 * q:32 * q + 32], wide)
    col_ids = strip0 + lax.broadcasted_iota(jnp.int32, (32, BLOCK), 0)
    row_ids = row0 + lax.broadcasted_iota(jnp.int32, (32, BLOCK), 1)

    @pl.when(both(neither(leading), NC * x + z // 8 <= NC * y + c))
    def _():
        wait(owned, own_r)
    schur = owned[...].reshape(32, BLOCK) * SCALE + jnp.where(col_ids == row_ids, damp, 0.0) - wide
    wide = jnp.where(leading, wide, schur)
    out_ref[...] = jnp.where(row_ids >= col_ids, wide, 0.0)

    for h in range(2):
        for sem in (0, 1, 2, 3, 4, 5):
            if sem in (0, 3) and h == 0 or sem in (1, 2) and h == 1 or sem == 4 + h:
                wait(part(x, h), g1_s.at[sem])
    for piece in range(NX):
        wait(feats.at[c, piece], sib_s.at[piece])
        for target in range(1, NY):
            @pl.when(target > y)
            def _():
                wait(slices.at[y, piece], sl_s.at[target, piece])
    for k in range(NY):
        sent_to_peers(k)
        owners(k, "finish")
    for k in moved:
        @pl.when(moved[k])
        def _():
            wait(partial.at[k], move_s.at[k])

    @pl.when(tracer)
    def _():
        wait(tz.at[pl.ds(0, NZ - 1)], tz_s)
        wait(many.at[pl.ds(0, PLANE - 1)], ty_s)

    @pl.when(hub)
    def _():
        @pl.loop(1, NY * NC)
        def _(i):
            wait(hubs, piv_s.at[i])

    @pl.when(holder)
    def _():
        wait(pin.at[pl.ds(0, STRIPS - 1)], p0_s)
        wait(pin.at[pl.ds(0, NZ - 1)], p1_s)

    @pl.when(both(hub, holder))
    def _():
        wait(gram.at[pl.ds(0, STRIPS - 1)], gz_s)
        for d in (1, 3, 2):
            wait(gpart, gx_s.at[d])
        wait(gin.at[pl.ds(0, NZ - 1)], hub_s)

    @pl.when(both(hub, neither(holder)))
    def _():
        wait(gram, gz_s)

    @pl.when(both(panel, neither(holder)))
    def _():
        wait(pin.at[pl.ds(0, STRIPS)], p0_s)
    pl.when(panel)(lambda: spread_panel(False))


def shards(a):
    dma = pltpu.SemaphoreType.DMA
    vmem = pl.BlockSpec(memory_space=pltpu.VMEM)
    result = pl.pallas_call(
        exchange,
        out_shape=jax.ShapeDtypeStruct((32, BLOCK), F32),
        in_specs=[vmem],
        out_specs=vmem,
        scratch_shapes=[
            pltpu.VMEM((NC, NX, BLOCK, BLOCK), BF16),
            pltpu.VMEM((NY, NX, SLICE, BLOCK), BF16),
            pltpu.VMEM((NY, STRIPS, NC, 8, BLOCK), F32),
            pltpu.VMEM((NY, NZ, NC, 8, BLOCK), F32),
            pltpu.VMEM((NY, NC, 8, BLOCK), F32),
            pltpu.VMEM((NZ, 8, BLOCK), F32),
            pltpu.VMEM((8, BLOCK), F32),
            pltpu.VMEM((NC, 4, 8, BLOCK), F32),
            pltpu.VMEM((NX, 4, 8, BLOCK), F32),
            pltpu.VMEM((NX, 8, 128), F32),
            pltpu.VMEM((STRIPS, 16, 128), F32),
            pltpu.VMEM((NX, 8, BLOCK), F32),
            pltpu.VMEM((NZ, 8, 128), F32),
            pltpu.VMEM((NY, 8, 128), F32),
            pltpu.VMEM((8, 128), F32),
            pltpu.VMEM((8, 128), F32),
            pltpu.VMEM((PANEL // 8, 2, 8, PANEL), F32),
            pltpu.VMEM((STRIPS, 16, 128), F32),
            pltpu.VMEM((8, 128), F32),
            pltpu.VMEM((PLANE, 8, 128), F32),
            pltpu.VMEM((STRIPS, 16, 128), F32),
            pltpu.VMEM((NZ, 16, 128), F32),
            pltpu.VMEM((16, 128), F32),
            pltpu.VMEM((NX, 16, 128), F32),
            pltpu.VMEM((16, 128), F32),
            dma((6,)), dma((NX, 2)),
            dma((NX,)), dma((NX,)),
            dma((NY, NX)), dma((NY, NX)),
            dma((NY,)), dma((NY,)),
            dma(()), dma(()),
            dma(()), dma(()),
            dma(()), dma(()),
            dma(()), dma(()),
            dma((NC, NX)), dma(()),
            dma((NY * NC,)), dma(()),
            dma((NY * NC,)), dma(()),
            dma((NY, NC)), dma(()),
            dma((NY,)), dma((NY,)),
            dma(()), dma(()),
            dma(()), dma(()),
            dma((NX,)), dma(()),
            pltpu.SemaphoreType.REGULAR((2,)),
        ],
        compiler_params=pltpu.CompilerParams(collective_id=0, has_side_effects=True),
    )(a)
    return result.T


def solution(mesh):
    finer = Mesh(mesh.devices.reshape(NX, NZ, NY, NC), ("x", "z", "y", "c"))
    return jax.shard_map(
        shards, mesh=finer, in_specs=(P(("x", "z"), ("y", "c")),), out_specs=P(("y", "c"), ("x", "z")), check_vma=False
    )
```

```python
import jax
import jax.numpy as jnp
from jax import lax
from jax.experimental import pallas as pl
from jax.experimental.pallas import tpu as pltpu
from jax.sharding import Mesh
from jax.sharding import PartitionSpec as P

MESH = pl.DeviceIdType.MESH
F32 = jnp.float32
BF16 = jnp.bfloat16
NX, NZ, NY, NC = 4, 16, 4, 2
BLOCK = 256
PANEL = 128
SLICE = BLOCK // NX
STRIPS = 8
FULL = BLOCK * NY * NC
TOKENS = BLOCK * NX * NZ
SCALE = 2.0 / TOKENS
PLANE = NX * NY * NC
GATES = 1
FIRST = 12

def wait(ref, sem):
    pltpu.make_async_copy(ref, ref, sem).wait()


def local(src, dst, sem):
    pltpu.make_async_copy(src, dst, sem).start()


def send(src, dst, send_sem, recv_sem, device):
    pltpu.make_async_remote_copy(
        src_ref=src,
        dst_ref=dst,
        send_sem=send_sem,
        recv_sem=recv_sem,
        device_id=device,
        device_id_type=MESH,
    ).start()


def far_first(i):
    return NZ // 2 + jnp.where(lax.rem(i, 2) == 0, i // 2, -((i + 1) // 2))


def both(*conditions):
    out = conditions[0]
    for condition in conditions[1:]:
        out = jnp.logical_and(out, condition)
    return out


def neither(condition):
    return jnp.logical_not(condition)


def spread_rows(row):
    return jnp.broadcast_to(row, (8, PANEL))


def spread_lane(tile, lane):
    return jnp.broadcast_to(tile[:, lane:lane + 1], (8, PANEL))


def eliminate(groups, first, last, sub):
    for k in range(first, last, 4):
        g0, r0 = k // 8, k % 8
        head = groups[g0]
        rows = [[spread_rows(head[h][r0 + i:r0 + i + 1]) for h in range(2)] for i in range(4)]
        dots = [[spread_lane(rows[i][0], k + j) if j >= i else None for j in range(4)] for i in range(4)]
        mults = [[None] * 4 for _ in range(4)]
        scaled = []
        for i in range(4):
            inv = 1.0 / dots[i][i]
            for j in range(i + 1, 4):
                mults[i][j] = dots[i][j] * inv
            for j in range(i + 1, 4):
                for l in range(j, 4):
                    dots[j][l] = dots[j][l] - mults[i][j] * dots[i][l]
                rows[j] = [rows[j][h] - mults[i][j] * rows[i][h] for h in range(2)]
            scaled.append([rows[i][h] * inv for h in range(2)])
        for i in (2, 1, 0):
            for j in range(i + 1, 4):
                scaled[i] = [scaled[i][h] - mults[i][j] * scaled[j][h] for h in range(2)]
        for g in range(g0 if r0 == 0 else g0 + 1, PANEL // 8):
            tile = groups[g]
            new = list(tile)
            for j in range(4):
                factor = spread_lane(tile[0], k + j)
                new = [new[h] - factor * scaled[j][h] for h in range(2)]
            if g == g0:
                new = [jnp.where(sub > 3, new[h], tile[h]) for h in range(2)]
            groups[g] = new
        for h in range(2):
            tile = groups[g0][h]
            for i in range(4):
                tile = jnp.where(sub == r0 + i, rows[i][h], tile)
            groups[g0] = [tile, groups[g0][1]] if h == 0 else [groups[g0][0], tile]


def exchange(a_ref, out_ref, feats, slices, partial, inbox, total, pin, psum, tall, rows, cols, pivot, owned,
             tz, ty, tq, tr, square, hubs, strip, many, gram, gin, gpart, gx, gtot, block_in,
             g1_s, g1_r, sib_s, sib_r, sl_s, sl_r, z_s, z_r, tz_s, tz_r, ty_s, ty_r, p0_s, p0_r, p1_s, p1_r,
             rows_s, rows_r, cols_s, cols_r, piv_s, piv_r, own_s, own_r, move_s, move_r, hub_s, hub_r, gz_s, gz_r, gx_s, gx_r, gate, in_sem):
    x, z, y, c = (lax.axis_index(name) for name in ("x", "z", "y", "c"))
    other = 1 - c

    def along(d):
        return (x, lax.rem(z + d + NZ, NZ), y, c)

    def in_plane(i):
        return (lax.rem(x + i // (NY * NC), NX), z, lax.rem(y + i // NC, NY), lax.rem(c + i, NC))

    barrier = pltpu.get_barrier_semaphore()

    local(a_ref, block_in, in_sem)

    @pl.loop(1, PLANE)
    def _(i):
        pl.semaphore_signal(barrier, inc=1, device_id=in_plane(i), device_id_type=MESH)

    @pl.loop(1, NZ)
    def _(d):
        pl.semaphore_signal(barrier, inc=1, device_id=along(d), device_id_type=MESH)

    wait(block_in, in_sem)
    feats[c, x] = block_in[...].T
    pl.semaphore_wait(barrier, PLANE - 1 + NZ - 1)
    hub = both(y == 0, c == 0)
    panel = c == 0
    place = lax.rem(z + NZ - FIRST, NZ)
    holder = both(panel, place < STRIPS)
    place_s, place_h = place // NC, lax.rem(place, NC)

    def part(piece, h):
        return feats.at[c, piece, pl.ds(128 * h, 128)]

    def pass_on(piece, h, step, sem):
        send(part(piece, h), part(piece, h), g1_s.at[sem], g1_r.at[piece, h], (lax.rem(x + step, NX), z, y, c))

    def relay(piece, h):
        send(part(piece, h), part(piece, h), sib_s.at[piece], sib_r.at[piece], (x, z, y, other))
        parts = []
        for k in range(4 * h, 4 * h + 4):
            start = pl.multiple_of(32 * k + 16 * (x // 2), 16)
            tile = feats[c, piece, pl.ds(start, 16)].astype(F32)
            parts.append(jnp.where(lax.rem(x, 2) == 1, tile[8:], tile[:8]))
        slices[y, piece, pl.ds(32 * h, 32)] = jnp.concatenate(parts, axis=0).astype(BF16)
        for target in range(1, NY):
            @pl.when(target > y)
            def _():
                there = slices.at[y, piece, pl.ds(32 * h, 32)]
                send(there, there, sl_s.at[target, piece], sl_r.at[y, piece], (x, z, target, c))

    pass_on(x, 0, 1, 0)
    pass_on(x, 1, 3, 1)
    pass_on(x, 1, 1, 2)
    pass_on(x, 0, 3, 3)
    relay(x, 0)
    relay(x, 1)

    def gram_out():
        block = feats[c, x, :PANEL]
        block = lax.dot_general(block, block, (((1,), (1,)), ((), ())), preferred_element_type=F32)
        gram[...] = block.reshape(STRIPS, 16, PANEL)
        for n in range(STRIPS):
            target = (FIRST + n) % NZ
            pl.when(target == z)(lambda: local(gram.at[n], gin.at[z], gz_r))
            pl.when(target != z)(lambda: send(gram.at[n], gin.at[z], gz_s, gz_r, (x, target, y, c)))

    left_x, right_x, far_x = lax.rem(x + 3, NX), lax.rem(x + 1, NX), lax.rem(x + 2, NX)
    for i, (piece, h, step) in enumerate(
        ((left_x, 0, 1), (right_x, 1, 3), (left_x, 1, 0), (right_x, 0, 0), (far_x, 0, 0), (far_x, 1, 0))
    ):
        wait(part(piece, h), g1_r.at[piece, h])
        if step:
            pass_on(piece, h, step, 4 + h)
        relay(piece, h)
        if i == 0:
            pl.when(hub)(gram_out)

    @pl.when(both(hub, holder))
    def _():
        wait(gin, gz_r)
        gpart[...] = jnp.sum(gin[...], axis=0)
        for d in (1, 3, 2):
            send(gpart, gx.at[x], gx_s.at[d], gx_r, (lax.rem(x + d, NX), z, y, c))
        local(gpart, gx.at[x], gx_r)
    for piece in range(NX):
        wait(feats.at[other, piece], sib_r.at[piece])

    moved = {2: y == 3}
    taken = {2: y == 0}
    gets = z // STRIPS == c

    def owner_row(k):
        return jnp.where(taken[k], NY - 1 - y, y) if k in taken else y

    def active(k):
        own = k <= y
        return jnp.logical_or(both(own, neither(moved[k])), taken[k]) if k in moved else own

    def halved(k):
        return both(c == 1, y == k)

    def first_strip(k):
        return jnp.where(panel, 4, 0) if k == 0 else 0

    def receives(k):
        return both(gets, active(k), lax.rem(z, STRIPS) >= first_strip(k))

    def arrived(source):
        @pl.when(source < y)
        def _():
            for piece in range(NX):
                wait(slices.at[source, piece], sl_r.at[source, piece])

    def multiply(source):
        for half in range(NC):
            acc = jnp.zeros((SLICE, BLOCK), F32)
            for piece in range(NX):
                acc += lax.dot_general(slices[source, piece], feats[half, piece], (((1,), (1,)), ((), ())),
                                       preferred_element_type=F32)
            for s in range(STRIPS):
                partial[source, s, half] = acc[8 * s:8 * s + 8]

    def reduce_to_peers(ks, when):
        @pl.loop(0, NZ)
        def _(i):
            target = lax.rem(z + jnp.where(i == NZ - 1, 0, far_first(i)), NZ)
            s = lax.rem(target, STRIPS)
            for k in ks:
                src, dst = partial.at[k, s], inbox.at[k, z]
                fits = both(when(k), target // STRIPS == c, s >= first_strip(k))

                def go(src, dst):
                    pl.when(target == z)(lambda: local(src, dst, z_r.at[k]))
                    pl.when(target != z)(lambda: send(src, dst, z_s.at[k], z_r.at[k], (x, target, y, c)))

                pl.when(both(fits, neither(halved(k))))(lambda: go(src, dst))
                pl.when(both(fits, halved(k)))(lambda: go(src.at[1], dst.at[1]))

    def sent_to_peers(k):
        count = STRIPS - first_strip(k) - jnp.where(receives(k), 1, 0)
        for n in (3, 4, 7, 8):
            if n < 5 and k > 0:
                continue

            @pl.when(both(active(k), count == n, neither(halved(k))))
            def _():
                wait(partial.at[k, pl.ds(0, n)], z_s.at[k])

            @pl.when(both(active(k), count == n, halved(k)))
            def _():
                wait(partial.at[k, pl.ds(0, n), 1], z_s.at[k])

    def owners(k, act):
        for half in range(NC):
            needed = receives(k) if half == 1 else both(receives(k), neither(halved(k)))
            here = both(k == x, owner_row(k) == y, half == c)

            if act == "start":
                pl.when(both(needed, here))(lambda: local(total.at[k, half], owned.at[x], own_r))

            @pl.when(both(needed, neither(here)))
            def _():
                if act == "start":
                    send(total.at[k, half], owned.at[x], own_s.at[k, half], own_r, (k, z, owner_row(k), half))
                else:
                    wait(total.at[k, half], own_s.at[k, half])

    def reduced(k):
        @pl.when(both(receives(k), neither(halved(k))))
        def _():
            wait(inbox.at[k], z_r.at[k])
            total[k] = jnp.sum(inbox[k], axis=0)

        @pl.when(both(receives(k), halved(k)))
        def _():
            wait(inbox.at[k, :, 1], z_r.at[k])
            total[k, 1] = jnp.sum(inbox[k, :, 1], axis=0)
        owners(k, "start")

    def taken_in(k):
        if k in taken:
            @pl.when(taken[k])
            def _():
                wait(partial.at[k], move_r.at[k])

    arrived(0)
    multiply(0)

    @pl.when(panel)
    def _():
        for n in range(STRIPS):
            target = (FIRST + n) % NZ

            @pl.when(target == z)
            def _():
                local(partial.at[0, n // NC, n % NC], pin.at[z], p0_r)

            @pl.when(target != z)
            def _():
                send(partial.at[0, n // NC, n % NC], pin.at[z], p0_s, p0_r, (x, target, y, c))

    @pl.when(both(hub, holder))
    def _():
        wait(gx, gx_r)
        gtot[...] = jnp.sum(gx[...], axis=0)

        for d in (8, 7, 9, 6, 10, 5, 11, 4, 12, 3, 13, 2, 14, 1, 15):
            send(gtot, hubs.at[place], hub_s, hub_r, along(d))
        local(gtot, hubs.at[place], hub_r)

    tracer = both(x == NX - 1, c == 1)

    @pl.when(tracer)
    def _():
        acc = jnp.zeros((8, 128), F32)
        for half in range(NC):
            for piece in range(NX):
                v = feats[half, piece].astype(F32)
                v = jnp.sum((v * v).reshape(BLOCK // 8, 8, BLOCK), axis=0)
                acc += v[:, :128] + v[:, 128:]
        tq[...] = acc

        @pl.loop(0, NZ - 1)
        def _(d):
            send(tq, tz.at[z], tz_s, tz_r, along(far_first(d)))
        local(tq, tz.at[z], tz_r)

    for k in (2, 3, 1):
        @pl.when(k <= y)
        def _():
            arrived(k)
            multiply(k)
        if k in moved:
            @pl.when(moved[k])
            def _():
                send(partial.at[k], partial.at[k], move_s.at[k], move_r.at[k], (x, z, NY - 1 - y, c))

    def kept(k):
        return both(active(k), neither(taken[k])) if k in taken else active(k)

    pl.when(panel)(lambda: reduce_to_peers((0, 1), kept))

    @pl.when(holder)
    def _():
        wait(pin, p0_r)
        psum[...] = jnp.sum(pin[...], axis=0)

        for d in (8, 7, 9, 6, 10, 5, 11, 4, 12, 3, 13, 2, 14, 1, 15):
            send(psum, tall.at[place_h, place_s], p1_s, p1_r, along(d))
        local(psum, tall.at[place_h, place_s], p1_r)

    pl.when(panel)(lambda: reduce_to_peers((2, 3), kept))

    @pl.when(neither(panel))
    def _():
        for n in range(GATES):
            pl.semaphore_signal(gate.at[n], inc=1, device_id=along(8), device_id_type=MESH)
            pl.semaphore_wait(gate.at[n], 1)
        reduce_to_peers((0, 1, 2, 3), kept)

    taken_in(2)
    pl.when(taken[2])(lambda: reduce_to_peers((2,), active))

    @pl.when(tracer)
    def _():
        wait(tz, tz_r)
        tr[...] = jnp.sum(tz[...], axis=0)

        @pl.loop(1, PLANE)
        def _(i):
            send(tr, ty.at[y], ty_s, ty_r, in_plane(i))
        local(tr, ty.at[y], ty_r)

    @pl.when(hub)
    def _():
        wait(hubs, hub_r)

        @pl.loop(1, NY * NC)
        def _(i):
            send(hubs, pivot, piv_s.at[i], piv_r, (x, z, lax.rem(y + i // NC, NY), lax.rem(c + i, NC)))
        local(hubs, pivot, piv_r)

    def spread(src, dst, sems, recv, count, where, start):
        for i in range(count):
            tx, to_y, tc = where(i)
            here = both(tx == x, to_y == y, tc == c)
            if start:
                pl.when(here)(lambda: local(src, dst, recv))
                pl.when(neither(here))(lambda: send(src, dst, sems.at[i], recv, (tx, z, to_y, tc)))
            else:
                pl.when(neither(here))(lambda: wait(src, sems.at[i]))

    def spread_panel(start):
        spread(strip, cols.at[x], cols_s, cols_r, NY * NC, lambda i: (y, i // 2, lax.rem(i, NC)), start)
        for half in range(NC):
            spread(tall.at[half], rows.at[x], rows_s.at[half], rows_r, NX, lambda i: (lax.rem(x + i, NX), y, half), start)

    @pl.when(panel)
    def _():
        wait(tall, p1_r)
        mixed = tall[z // 8].reshape(32, BLOCK)
        mixed = jnp.where(lax.rem(z, 8) >= 4, mixed[:, 128:], mixed[:, :128])
        lanes = lax.broadcasted_iota(jnp.int32, (8, 128), 1) // 32
        packed = jnp.zeros((8, 128), F32)
        for q in range(4):
            turned = pltpu.roll(mixed[8 * q:8 * q + 8], lax.rem(32 * q - 32 * lax.rem(z, 4) + 128, 128), 1)
            packed = jnp.where(lanes == q, turned, packed)
        strip[...] = packed
        spread_panel(True)

    wait(pivot, piv_r)
    wait(ty, ty_r)
    damp = jnp.sum(jnp.sum(ty[...], axis=0), keepdims=True) * (SCALE * 0.01 / FULL)
    lane = lax.broadcasted_iota(jnp.int32, (8, PANEL), 1)
    sub = lax.broadcasted_iota(jnp.int32, (8, PANEL), 0)
    groups = []
    for g in range(PANEL // 8):
        diag = lane == sub + 8 * g
        left = pivot[g // 2, 8 * (g % 2):8 * (g % 2) + 8] * SCALE + jnp.where(diag, damp, 0.0)
        groups.append([left, jnp.where(diag, 1.0, 0.0).astype(F32)])
    eliminate(groups, 0, PANEL // 2, sub)
    for g in range(PANEL // 8):
        square[g, 0] = groups[g][0]
        square[g, 1] = groups[g][1]
    for k in range(NY):
        reduced(k)
    groups = [[square[g, 0], square[g, 1]] for g in range(PANEL // 8)]
    eliminate(groups, PANEL // 2, PANEL, sub)
    scaled = []
    for g in range(PANEL // 8):
        diag = jnp.sum(jnp.where(lane == sub + 8 * g, groups[g][0], 0.0), axis=1, keepdims=True)
        scaled.append(groups[g][1] * lax.rsqrt(diag))
    inverse = jnp.concatenate(scaled, axis=0)
    highest = lax.Precision.HIGHEST
    wait(cols, cols_r)
    left = jnp.concatenate([pltpu.roll(cols[i], (128 - 32 * q) % 128, 1) for q in range(4) for i in range(NX)], axis=0)
    left = jnp.dot(inverse, left * SCALE, precision=highest, preferred_element_type=F32)[:, :32]
    wait(rows, rows_r)
    ids = lax.broadcasted_iota(jnp.int32, (PANEL, BLOCK), 0)
    row0 = (y * NC + c) * BLOCK
    row_ids = row0 + lax.broadcasted_iota(jnp.int32, (PANEL, BLOCK), 1)
    right = jnp.concatenate([rows[i, q] for q in range(4) for i in range(NX)], axis=0)
    right = right * SCALE + jnp.where(ids == row_ids, damp, 0.0)
    right = jnp.dot(inverse, right, precision=highest, preferred_element_type=F32)
    update = lax.dot_general(left, right, (((0,), (0,)), ((), ())), precision=highest, preferred_element_type=F32)
    strip0 = (x * NZ + z) * 32
    leading = strip0 < PANEL
    wide = update
    for q in range(4):
        wide = jnp.where(both(leading, z == q), right[32 * q:32 * q + 32], wide)
    col_ids = strip0 + lax.broadcasted_iota(jnp.int32, (32, BLOCK), 0)
    row_ids = row0 + lax.broadcasted_iota(jnp.int32, (32, BLOCK), 1)

    @pl.when(both(neither(leading), NC * x + z // 8 <= NC * y + c))
    def _():
        wait(owned, own_r)
    schur = owned[...].reshape(32, BLOCK) * SCALE + jnp.where(col_ids == row_ids, damp, 0.0) - wide
    wide = jnp.where(leading, wide, schur)
    out_ref[...] = jnp.where(row_ids >= col_ids, wide, 0.0)

    for h in range(2):
        for sem in (0, 1, 2, 3, 4, 5):
            if sem in (0, 3) and h == 0 or sem in (1, 2) and h == 1 or sem == 4 + h:
                wait(part(x, h), g1_s.at[sem])
    for piece in range(NX):
        wait(feats.at[c, piece], sib_s.at[piece])
        for target in range(1, NY):
            @pl.when(target > y)
            def _():
                wait(slices.at[y, piece], sl_s.at[target, piece])
    for k in range(NY):
        sent_to_peers(k)
        owners(k, "finish")
    for k in moved:
        @pl.when(moved[k])
        def _():
            wait(partial.at[k], move_s.at[k])

    @pl.when(tracer)
    def _():
        wait(tz.at[pl.ds(0, NZ - 1)], tz_s)
        wait(many.at[pl.ds(0, PLANE - 1)], ty_s)

    @pl.when(hub)
    def _():
        @pl.loop(1, NY * NC)
        def _(i):
            wait(hubs, piv_s.at[i])

    @pl.when(holder)
    def _():
        wait(pin.at[pl.ds(0, STRIPS - 1)], p0_s)
        wait(pin.at[pl.ds(0, NZ - 1)], p1_s)

    @pl.when(both(hub, holder))
    def _():
        wait(gram.at[pl.ds(0, STRIPS - 1)], gz_s)
        for d in (1, 3, 2):
            wait(gpart, gx_s.at[d])
        wait(gin.at[pl.ds(0, NZ - 1)], hub_s)

    @pl.when(both(hub, neither(holder)))
    def _():
        wait(gram, gz_s)

    @pl.when(both(panel, neither(holder)))
    def _():
        wait(pin.at[pl.ds(0, STRIPS)], p0_s)
    pl.when(panel)(lambda: spread_panel(False))


def shards(a):
    dma = pltpu.SemaphoreType.DMA
    vmem = pl.BlockSpec(memory_space=pltpu.VMEM)
    result = pl.pallas_call(
        exchange,
        out_shape=jax.ShapeDtypeStruct((32, BLOCK), F32),
        in_specs=[pl.BlockSpec(memory_space=pl.ANY)],
        out_specs=vmem,
        scratch_shapes=[
            pltpu.VMEM((NC, NX, BLOCK, BLOCK), BF16),
            pltpu.VMEM((NY, NX, SLICE, BLOCK), BF16),
            pltpu.VMEM((NY, STRIPS, NC, 8, BLOCK), F32),
            pltpu.VMEM((NY, NZ, NC, 8, BLOCK), F32),
            pltpu.VMEM((NY, NC, 8, BLOCK), F32),
            pltpu.VMEM((NZ, 8, BLOCK), F32),
            pltpu.VMEM((8, BLOCK), F32),
            pltpu.VMEM((NC, 4, 8, BLOCK), F32),
            pltpu.VMEM((NX, 4, 8, BLOCK), F32),
            pltpu.VMEM((NX, 8, 128), F32),
            pltpu.VMEM((STRIPS, 16, 128), F32),
            pltpu.VMEM((NX, 8, BLOCK), F32),
            pltpu.VMEM((NZ, 8, 128), F32),
            pltpu.VMEM((NY, 8, 128), F32),
            pltpu.VMEM((8, 128), F32),
            pltpu.VMEM((8, 128), F32),
            pltpu.VMEM((PANEL // 8, 2, 8, PANEL), F32),
            pltpu.VMEM((STRIPS, 16, 128), F32),
            pltpu.VMEM((8, 128), F32),
            pltpu.VMEM((PLANE, 8, 128), F32),
            pltpu.VMEM((STRIPS, 16, 128), F32),
            pltpu.VMEM((NZ, 16, 128), F32),
            pltpu.VMEM((16, 128), F32),
            pltpu.VMEM((NX, 16, 128), F32),
            pltpu.VMEM((16, 128), F32),
            pltpu.VMEM((BLOCK, BLOCK), BF16),
            dma((6,)), dma((NX, 2)),
            dma((NX,)), dma((NX,)),
            dma((NY, NX)), dma((NY, NX)),
            dma((NY,)), dma((NY,)),
            dma(()), dma(()),
            dma(()), dma(()),
            dma(()), dma(()),
            dma(()), dma(()),
            dma((NC, NX)), dma(()),
            dma((NY * NC,)), dma(()),
            dma((NY * NC,)), dma(()),
            dma((NY, NC)), dma(()),
            dma((NY,)), dma((NY,)),
            dma(()), dma(()),
            dma(()), dma(()),
            dma((NX,)), dma(()),
            pltpu.SemaphoreType.REGULAR((1,)),
            dma(()),
        ],
        compiler_params=pltpu.CompilerParams(collective_id=0, has_side_effects=True),
    )(a)
    return result.T


def solution(mesh):
    finer = Mesh(mesh.devices.reshape(NX, NZ, NY, NC), ("x", "z", "y", "c"))
    return jax.shard_map(
        shards, mesh=finer, in_specs=(P(("x", "z"), ("y", "c")),), out_specs=P(("y", "c"), ("x", "z")), check_vma=False
    )
```

```python
import jax
import jax.numpy as jnp
from jax import lax
from jax.experimental import pallas as pl
from jax.experimental.pallas import tpu as pltpu
from jax.sharding import Mesh
from jax.sharding import PartitionSpec as P

MESH = pl.DeviceIdType.MESH
F32 = jnp.float32
BF16 = jnp.bfloat16
NX, NZ, NY, NC = 4, 16, 4, 2
BLOCK = 256
PANEL = 128
SLICE = BLOCK // NX
STRIPS = 8
FULL = BLOCK * NY * NC
TOKENS = BLOCK * NX * NZ
SCALE = 2.0 / TOKENS
PLANE = NX * NY * NC
GATES = 1
FIRST = 12

def wait(ref, sem):
    pltpu.make_async_copy(ref, ref, sem).wait()


def local(src, dst, sem):
    pltpu.make_async_copy(src, dst, sem).start()


def send(src, dst, send_sem, recv_sem, device):
    pltpu.make_async_remote_copy(
        src_ref=src,
        dst_ref=dst,
        send_sem=send_sem,
        recv_sem=recv_sem,
        device_id=device,
        device_id_type=MESH,
    ).start()


def far_first(i):
    return NZ // 2 + jnp.where(lax.rem(i, 2) == 0, i // 2, -((i + 1) // 2))


def both(*conditions):
    out = conditions[0]
    for condition in conditions[1:]:
        out = jnp.logical_and(out, condition)
    return out


def neither(condition):
    return jnp.logical_not(condition)


def spread_rows(row):
    return jnp.broadcast_to(row, (8, PANEL))


def spread_lane(tile, lane):
    return jnp.broadcast_to(tile[:, lane:lane + 1], (8, PANEL))


def eliminate(groups, first, last, sub):
    for k in range(first, last, 4):
        g0, r0 = k // 8, k % 8
        head = groups[g0]
        rows = [[spread_rows(head[h][r0 + i:r0 + i + 1]) for h in range(2)] for i in range(4)]
        dots = [[spread_lane(rows[i][0], k + j) if j >= i else None for j in range(4)] for i in range(4)]
        mults = [[None] * 4 for _ in range(4)]
        scaled = []
        for i in range(4):
            inv = 1.0 / dots[i][i]
            for j in range(i + 1, 4):
                mults[i][j] = dots[i][j] * inv
            for j in range(i + 1, 4):
                for l in range(j, 4):
                    dots[j][l] = dots[j][l] - mults[i][j] * dots[i][l]
                rows[j] = [rows[j][h] - mults[i][j] * rows[i][h] for h in range(2)]
            scaled.append([rows[i][h] * inv for h in range(2)])
        for i in (2, 1, 0):
            for j in range(i + 1, 4):
                scaled[i] = [scaled[i][h] - mults[i][j] * scaled[j][h] for h in range(2)]
        for g in range(g0 if r0 == 0 else g0 + 1, PANEL // 8):
            tile = groups[g]
            new = list(tile)
            for j in range(4):
                factor = spread_lane(tile[0], k + j)
                new = [new[h] - factor * scaled[j][h] for h in range(2)]
            if g == g0:
                new = [jnp.where(sub > 3, new[h], tile[h]) for h in range(2)]
            groups[g] = new
        for h in range(2):
            tile = groups[g0][h]
            for i in range(4):
                tile = jnp.where(sub == r0 + i, rows[i][h], tile)
            groups[g0] = [tile, groups[g0][1]] if h == 0 else [groups[g0][0], tile]


def exchange(a_ref, out_ref, feats, slices, partial, inbox, total, pin, psum, tall, rows, cols, pivot, owned,
             tz, ty, tq, tr, square, hubs, strip, many, gram, gin, gpart, gx, gtot, block_in,
             g1_s, g1_r, sib_s, sib_r, sl_s, sl_r, z_s, z_r, tz_s, tz_r, ty_s, ty_r, p0_s, p0_r, p1_s, p1_r,
             rows_s, rows_r, cols_s, cols_r, piv_s, piv_r, own_s, own_r, move_s, move_r, hub_s, hub_r, gz_s, gz_r, gx_s, gx_r, gate, in_sem):
    x, z, y, c = (lax.axis_index(name) for name in ("x", "z", "y", "c"))
    other = 1 - c

    def along(d):
        return (x, lax.rem(z + d + NZ, NZ), y, c)

    def in_plane(i):
        return (lax.rem(x + i // (NY * NC), NX), z, lax.rem(y + i // NC, NY), lax.rem(c + i, NC))

    barrier = pltpu.get_barrier_semaphore()

    local(a_ref, block_in, in_sem)

    @pl.loop(1, PLANE)
    def _(i):
        pl.semaphore_signal(barrier, inc=1, device_id=in_plane(i), device_id_type=MESH)

    @pl.loop(1, NZ)
    def _(d):
        pl.semaphore_signal(barrier, inc=1, device_id=along(d), device_id_type=MESH)

    wait(block_in, in_sem)
    feats[c, x] = block_in[...].T
    pl.semaphore_wait(barrier, PLANE - 1 + NZ - 1)
    hub = both(y == 0, c == 0)
    panel = c == 0
    place = lax.rem(z + NZ - FIRST, NZ)
    holder = both(panel, place < STRIPS)
    place_s, place_h = place // NC, lax.rem(place, NC)

    def part(piece, h):
        return feats.at[c, piece, pl.ds(128 * h, 128)]

    def pass_on(piece, h, step, sem):
        send(part(piece, h), part(piece, h), g1_s.at[sem], g1_r.at[piece, h], (lax.rem(x + step, NX), z, y, c))

    def relay(piece, h):
        send(part(piece, h), part(piece, h), sib_s.at[piece], sib_r.at[piece], (x, z, y, other))
        parts = []
        for k in range(4 * h, 4 * h + 4):
            start = pl.multiple_of(32 * k + 16 * (x // 2), 16)
            tile = feats[c, piece, pl.ds(start, 16)].astype(F32)
            parts.append(jnp.where(lax.rem(x, 2) == 1, tile[8:], tile[:8]))
        slices[y, piece, pl.ds(32 * h, 32)] = jnp.concatenate(parts, axis=0).astype(BF16)
        for target in range(1, NY):
            @pl.when(target > y)
            def _():
                there = slices.at[y, piece, pl.ds(32 * h, 32)]
                send(there, there, sl_s.at[target, piece], sl_r.at[y, piece], (x, z, target, c))

    pass_on(x, 0, 1, 0)
    pass_on(x, 1, 3, 1)
    pass_on(x, 1, 1, 2)
    pass_on(x, 0, 3, 3)
    relay(x, 0)
    relay(x, 1)

    def gram_out():
        block = feats[c, x, :PANEL]
        block = lax.dot_general(block, block, (((1,), (1,)), ((), ())), preferred_element_type=F32)
        gram[...] = block.reshape(STRIPS, 16, PANEL)
        for n in range(STRIPS):
            target = (FIRST + n) % NZ
            pl.when(target == z)(lambda: local(gram.at[n], gin.at[z], gz_r))
            pl.when(target != z)(lambda: send(gram.at[n], gin.at[z], gz_s, gz_r, (x, target, y, c)))

    left_x, right_x, far_x = lax.rem(x + 3, NX), lax.rem(x + 1, NX), lax.rem(x + 2, NX)
    for i, (piece, h, step) in enumerate(
        ((left_x, 0, 1), (right_x, 1, 3), (left_x, 1, 0), (right_x, 0, 0), (far_x, 0, 0), (far_x, 1, 0))
    ):
        wait(part(piece, h), g1_r.at[piece, h])
        if step:
            pass_on(piece, h, step, 4 + h)
        relay(piece, h)
        if i == 0:
            pl.when(hub)(gram_out)

    @pl.when(both(hub, holder))
    def _():
        wait(gin, gz_r)
        gpart[...] = jnp.sum(gin[...], axis=0)
        for d in (1, 3, 2):
            send(gpart, gx.at[x], gx_s.at[d], gx_r, (lax.rem(x + d, NX), z, y, c))
        local(gpart, gx.at[x], gx_r)
    for piece in range(NX):
        wait(feats.at[other, piece], sib_r.at[piece])

    moved = {2: y == 3}
    taken = {2: y == 0}
    gets = z // STRIPS == c

    def owner_row(k):
        return jnp.where(taken[k], NY - 1 - y, y) if k in taken else y

    def active(k):
        own = k <= y
        return jnp.logical_or(both(own, neither(moved[k])), taken[k]) if k in moved else own

    def halved(k):
        return both(c == 1, y == k)

    def first_strip(k):
        return jnp.where(panel, 4, 0) if k == 0 else 0

    def receives(k):
        return both(gets, active(k), lax.rem(z, STRIPS) >= first_strip(k))

    def arrived(source):
        @pl.when(source < y)
        def _():
            for piece in range(NX):
                wait(slices.at[source, piece], sl_r.at[source, piece])

    def multiply(source):
        for half in range(NC):
            acc = jnp.zeros((SLICE, BLOCK), F32)
            for piece in range(NX):
                acc += lax.dot_general(slices[source, piece], feats[half, piece], (((1,), (1,)), ((), ())),
                                       preferred_element_type=F32)
            for s in range(STRIPS):
                partial[source, s, half] = acc[8 * s:8 * s + 8]

    def reduce_to_peers(ks, when):
        @pl.loop(0, NZ)
        def _(i):
            target = lax.rem(z + jnp.where(i == NZ - 1, 0, far_first(i)), NZ)
            s = lax.rem(target, STRIPS)
            for k in ks:
                src, dst = partial.at[k, s], inbox.at[k, z]
                fits = both(when(k), target // STRIPS == c, s >= first_strip(k))

                def go(src, dst):
                    pl.when(target == z)(lambda: local(src, dst, z_r.at[k]))
                    pl.when(target != z)(lambda: send(src, dst, z_s.at[k], z_r.at[k], (x, target, y, c)))

                pl.when(both(fits, neither(halved(k))))(lambda: go(src, dst))
                pl.when(both(fits, halved(k)))(lambda: go(src.at[1], dst.at[1]))

    def sent_to_peers(k):
        count = STRIPS - first_strip(k) - jnp.where(receives(k), 1, 0)
        for n in (3, 4, 7, 8):
            if n < 5 and k > 0:
                continue

            @pl.when(both(active(k), count == n, neither(halved(k))))
            def _():
                wait(partial.at[k, pl.ds(0, n)], z_s.at[k])

            @pl.when(both(active(k), count == n, halved(k)))
            def _():
                wait(partial.at[k, pl.ds(0, n), 1], z_s.at[k])

    def owners(k, act):
        for half in range(NC):
            needed = receives(k) if half == 1 else both(receives(k), neither(halved(k)))
            here = both(k == x, owner_row(k) == y, half == c)

            if act == "start":
                pl.when(both(needed, here))(lambda: local(total.at[k, half], owned.at[x], own_r))

            @pl.when(both(needed, neither(here)))
            def _():
                if act == "start":
                    send(total.at[k, half], owned.at[x], own_s.at[k, half], own_r, (k, z, owner_row(k), half))
                else:
                    wait(total.at[k, half], own_s.at[k, half])

    def reduced(k):
        @pl.when(both(receives(k), neither(halved(k))))
        def _():
            wait(inbox.at[k], z_r.at[k])
            total[k] = jnp.sum(inbox[k], axis=0)

        @pl.when(both(receives(k), halved(k)))
        def _():
            wait(inbox.at[k, :, 1], z_r.at[k])
            total[k, 1] = jnp.sum(inbox[k, :, 1], axis=0)
        owners(k, "start")

    def taken_in(k):
        if k in taken:
            @pl.when(taken[k])
            def _():
                wait(partial.at[k], move_r.at[k])

    arrived(0)
    multiply(0)

    @pl.when(panel)
    def _():
        for n in range(STRIPS):
            target = (FIRST + n) % NZ

            @pl.when(target == z)
            def _():
                local(partial.at[0, n // NC, n % NC], pin.at[z], p0_r)

            @pl.when(target != z)
            def _():
                send(partial.at[0, n // NC, n % NC], pin.at[z], p0_s, p0_r, (x, target, y, c))

    @pl.when(both(hub, holder))
    def _():
        wait(gx, gx_r)
        gtot[...] = jnp.sum(gx[...], axis=0)

        for d in (8, 7, 9, 6, 10, 5, 11, 4, 12, 3, 13, 2, 14, 1, 15):
            send(gtot, hubs.at[place], hub_s, hub_r, along(d))
        local(gtot, hubs.at[place], hub_r)

    tracer = both(x == NX - 1, c == 1)

    @pl.when(tracer)
    def _():
        acc = jnp.zeros((8, 128), F32)
        for half in range(NC):
            for piece in range(NX):
                v = feats[half, piece].astype(F32)
                v = jnp.sum((v * v).reshape(BLOCK // 8, 8, BLOCK), axis=0)
                acc += v[:, :128] + v[:, 128:]
        tq[...] = acc

        @pl.loop(0, NZ - 1)
        def _(d):
            send(tq, tz.at[z], tz_s, tz_r, along(far_first(d)))
        local(tq, tz.at[z], tz_r)

    for k in (2, 3, 1):
        @pl.when(k <= y)
        def _():
            arrived(k)
            multiply(k)
        if k in moved:
            @pl.when(moved[k])
            def _():
                send(partial.at[k], partial.at[k], move_s.at[k], move_r.at[k], (x, z, NY - 1 - y, c))

    def kept(k):
        return both(active(k), neither(taken[k])) if k in taken else active(k)

    pl.when(panel)(lambda: reduce_to_peers((0, 1), kept))

    @pl.when(holder)
    def _():
        wait(pin, p0_r)
        psum[...] = jnp.sum(pin[...], axis=0)

        for d in (8, 7, 9, 6, 10, 5, 11, 4, 12, 3, 13, 2, 14, 1, 15):
            send(psum, tall.at[place_h, place_s], p1_s, p1_r, along(d))
        local(psum, tall.at[place_h, place_s], p1_r)

    pl.when(panel)(lambda: reduce_to_peers((2, 3), kept))

    @pl.when(neither(panel))
    def _():
        for n in range(GATES):
            pl.semaphore_signal(gate.at[n], inc=1, device_id=along(8), device_id_type=MESH)
            pl.semaphore_wait(gate.at[n], 1)
        for k in range(NY):
            reduce_to_peers((k,), kept)

    taken_in(2)
    pl.when(taken[2])(lambda: reduce_to_peers((2,), active))

    @pl.when(tracer)
    def _():
        wait(tz, tz_r)
        tr[...] = jnp.sum(tz[...], axis=0)

        @pl.loop(1, PLANE)
        def _(i):
            send(tr, ty.at[y], ty_s, ty_r, in_plane(i))
        local(tr, ty.at[y], ty_r)

    @pl.when(hub)
    def _():
        wait(hubs, hub_r)

        @pl.loop(1, NY * NC)
        def _(i):
            send(hubs, pivot, piv_s.at[i], piv_r, (x, z, lax.rem(y + i // NC, NY), lax.rem(c + i, NC)))
        local(hubs, pivot, piv_r)

    def spread(src, dst, sems, recv, count, where, start):
        for i in range(count):
            tx, to_y, tc = where(i)
            here = both(tx == x, to_y == y, tc == c)
            if start:
                pl.when(here)(lambda: local(src, dst, recv))
                pl.when(neither(here))(lambda: send(src, dst, sems.at[i], recv, (tx, z, to_y, tc)))
            else:
                pl.when(neither(here))(lambda: wait(src, sems.at[i]))

    def spread_panel(start):
        spread(strip, cols.at[x], cols_s, cols_r, NY * NC, lambda i: (y, i // 2, lax.rem(i, NC)), start)
        for half in range(NC):
            spread(tall.at[half], rows.at[x], rows_s.at[half], rows_r, NX, lambda i: (lax.rem(x + i, NX), y, half), start)

    @pl.when(panel)
    def _():
        wait(tall, p1_r)
        mixed = tall[z // 8].reshape(32, BLOCK)
        mixed = jnp.where(lax.rem(z, 8) >= 4, mixed[:, 128:], mixed[:, :128])
        lanes = lax.broadcasted_iota(jnp.int32, (8, 128), 1) // 32
        packed = jnp.zeros((8, 128), F32)
        for q in range(4):
            turned = pltpu.roll(mixed[8 * q:8 * q + 8], lax.rem(32 * q - 32 * lax.rem(z, 4) + 128, 128), 1)
            packed = jnp.where(lanes == q, turned, packed)
        strip[...] = packed
        spread_panel(True)

    wait(pivot, piv_r)
    wait(ty, ty_r)
    damp = jnp.sum(jnp.sum(ty[...], axis=0), keepdims=True) * (SCALE * 0.01 / FULL)
    lane = lax.broadcasted_iota(jnp.int32, (8, PANEL), 1)
    sub = lax.broadcasted_iota(jnp.int32, (8, PANEL), 0)
    groups = []
    for g in range(PANEL // 8):
        diag = lane == sub + 8 * g
        left = pivot[g // 2, 8 * (g % 2):8 * (g % 2) + 8] * SCALE + jnp.where(diag, damp, 0.0)
        groups.append([left, jnp.where(diag, 1.0, 0.0).astype(F32)])
    eliminate(groups, 0, PANEL // 2, sub)
    for g in range(PANEL // 8):
        square[g, 0] = groups[g][0]
        square[g, 1] = groups[g][1]
    for k in range(NY):
        reduced(k)
    groups = [[square[g, 0], square[g, 1]] for g in range(PANEL // 8)]
    eliminate(groups, PANEL // 2, PANEL, sub)
    scaled = []
    for g in range(PANEL // 8):
        diag = jnp.sum(jnp.where(lane == sub + 8 * g, groups[g][0], 0.0), axis=1, keepdims=True)
        scaled.append(groups[g][1] * lax.rsqrt(diag))
    inverse = jnp.concatenate(scaled, axis=0)
    highest = lax.Precision.HIGHEST
    wait(cols, cols_r)
    left = jnp.concatenate([pltpu.roll(cols[i], (128 - 32 * q) % 128, 1) for q in range(4) for i in range(NX)], axis=0)
    left = jnp.dot(inverse, left * SCALE, precision=highest, preferred_element_type=F32)[:, :32]
    wait(rows, rows_r)
    ids = lax.broadcasted_iota(jnp.int32, (PANEL, BLOCK), 0)
    row0 = (y * NC + c) * BLOCK
    row_ids = row0 + lax.broadcasted_iota(jnp.int32, (PANEL, BLOCK), 1)
    right = jnp.concatenate([rows[i, q] for q in range(4) for i in range(NX)], axis=0)
    right = right * SCALE + jnp.where(ids == row_ids, damp, 0.0)
    right = jnp.dot(inverse, right, precision=highest, preferred_element_type=F32)
    update = lax.dot_general(left, right, (((0,), (0,)), ((), ())), precision=highest, preferred_element_type=F32)
    strip0 = (x * NZ + z) * 32
    leading = strip0 < PANEL
    wide = update
    for q in range(4):
        wide = jnp.where(both(leading, z == q), right[32 * q:32 * q + 32], wide)
    col_ids = strip0 + lax.broadcasted_iota(jnp.int32, (32, BLOCK), 0)
    row_ids = row0 + lax.broadcasted_iota(jnp.int32, (32, BLOCK), 1)

    @pl.when(both(neither(leading), NC * x + z // 8 <= NC * y + c))
    def _():
        wait(owned, own_r)
    schur = owned[...].reshape(32, BLOCK) * SCALE + jnp.where(col_ids == row_ids, damp, 0.0) - wide
    wide = jnp.where(leading, wide, schur)
    out_ref[...] = jnp.where(row_ids >= col_ids, wide, 0.0)

    for h in range(2):
        for sem in (0, 1, 2, 3, 4, 5):
            if sem in (0, 3) and h == 0 or sem in (1, 2) and h == 1 or sem == 4 + h:
                wait(part(x, h), g1_s.at[sem])
    for piece in range(NX):
        wait(feats.at[c, piece], sib_s.at[piece])
        for target in range(1, NY):
            @pl.when(target > y)
            def _():
                wait(slices.at[y, piece], sl_s.at[target, piece])
    for k in range(NY):
        sent_to_peers(k)
        owners(k, "finish")
    for k in moved:
        @pl.when(moved[k])
        def _():
            wait(partial.at[k], move_s.at[k])

    @pl.when(tracer)
    def _():
        wait(tz.at[pl.ds(0, NZ - 1)], tz_s)
        wait(many.at[pl.ds(0, PLANE - 1)], ty_s)

    @pl.when(hub)
    def _():
        @pl.loop(1, NY * NC)
        def _(i):
            wait(hubs, piv_s.at[i])

    @pl.when(holder)
    def _():
        wait(pin.at[pl.ds(0, STRIPS - 1)], p0_s)
        wait(pin.at[pl.ds(0, NZ - 1)], p1_s)

    @pl.when(both(hub, holder))
    def _():
        wait(gram.at[pl.ds(0, STRIPS - 1)], gz_s)
        for d in (1, 3, 2):
            wait(gpart, gx_s.at[d])
        wait(gin.at[pl.ds(0, NZ - 1)], hub_s)

    @pl.when(both(hub, neither(holder)))
    def _():
        wait(gram, gz_s)

    @pl.when(both(panel, neither(holder)))
    def _():
        wait(pin.at[pl.ds(0, STRIPS)], p0_s)
    pl.when(panel)(lambda: spread_panel(False))


def shards(a):
    dma = pltpu.SemaphoreType.DMA
    vmem = pl.BlockSpec(memory_space=pltpu.VMEM)
    result = pl.pallas_call(
        exchange,
        out_shape=jax.ShapeDtypeStruct((32, BLOCK), F32),
        in_specs=[pl.BlockSpec(memory_space=pl.ANY)],
        out_specs=vmem,
        scratch_shapes=[
            pltpu.VMEM((NC, NX, BLOCK, BLOCK), BF16),
            pltpu.VMEM((NY, NX, SLICE, BLOCK), BF16),
            pltpu.VMEM((NY, STRIPS, NC, 8, BLOCK), F32),
            pltpu.VMEM((NY, NZ, NC, 8, BLOCK), F32),
            pltpu.VMEM((NY, NC, 8, BLOCK), F32),
            pltpu.VMEM((NZ, 8, BLOCK), F32),
            pltpu.VMEM((8, BLOCK), F32),
            pltpu.VMEM((NC, 4, 8, BLOCK), F32),
            pltpu.VMEM((NX, 4, 8, BLOCK), F32),
            pltpu.VMEM((NX, 8, 128), F32),
            pltpu.VMEM((STRIPS, 16, 128), F32),
            pltpu.VMEM((NX, 8, BLOCK), F32),
            pltpu.VMEM((NZ, 8, 128), F32),
            pltpu.VMEM((NY, 8, 128), F32),
            pltpu.VMEM((8, 128), F32),
            pltpu.VMEM((8, 128), F32),
            pltpu.VMEM((PANEL // 8, 2, 8, PANEL), F32),
            pltpu.VMEM((STRIPS, 16, 128), F32),
            pltpu.VMEM((8, 128), F32),
            pltpu.VMEM((PLANE, 8, 128), F32),
            pltpu.VMEM((STRIPS, 16, 128), F32),
            pltpu.VMEM((NZ, 16, 128), F32),
            pltpu.VMEM((16, 128), F32),
            pltpu.VMEM((NX, 16, 128), F32),
            pltpu.VMEM((16, 128), F32),
            pltpu.VMEM((BLOCK, BLOCK), BF16),
            dma((6,)), dma((NX, 2)),
            dma((NX,)), dma((NX,)),
            dma((NY, NX)), dma((NY, NX)),
            dma((NY,)), dma((NY,)),
            dma(()), dma(()),
            dma(()), dma(()),
            dma(()), dma(()),
            dma(()), dma(()),
            dma((NC, NX)), dma(()),
            dma((NY * NC,)), dma(()),
            dma((NY * NC,)), dma(()),
            dma((NY, NC)), dma(()),
            dma((NY,)), dma((NY,)),
            dma(()), dma(()),
            dma(()), dma(()),
            dma((NX,)), dma(()),
            pltpu.SemaphoreType.REGULAR((1,)),
            dma(()),
        ],
        compiler_params=pltpu.CompilerParams(collective_id=0, has_side_effects=True),
    )(a)
    return result.T


def solution(mesh):
    finer = Mesh(mesh.devices.reshape(NX, NZ, NY, NC), ("x", "z", "y", "c"))
    return jax.shard_map(
        shards, mesh=finer, in_specs=(P(("x", "z"), ("y", "c")),), out_specs=P(("y", "c"), ("x", "z")), check_vma=False
    )
```

```python
import jax
import jax.numpy as jnp
from jax import lax
from jax.experimental import pallas as pl
from jax.experimental.pallas import tpu as pltpu
from jax.sharding import Mesh
from jax.sharding import PartitionSpec as P

MESH = pl.DeviceIdType.MESH
F32 = jnp.float32
BF16 = jnp.bfloat16
NX, NZ, NY, NC = 4, 16, 4, 2
BLOCK = 256
PANEL = 128
SLICE = BLOCK // NX
STRIPS = 8
FULL = BLOCK * NY * NC
TOKENS = BLOCK * NX * NZ
SCALE = 2.0 / TOKENS
PLANE = NX * NY * NC
GATES = 1
FIRST = 12

def wait(ref, sem):
    pltpu.make_async_copy(ref, ref, sem).wait()


def local(src, dst, sem):
    pltpu.make_async_copy(src, dst, sem).start()


def send(src, dst, send_sem, recv_sem, device):
    pltpu.make_async_remote_copy(
        src_ref=src,
        dst_ref=dst,
        send_sem=send_sem,
        recv_sem=recv_sem,
        device_id=device,
        device_id_type=MESH,
    ).start()


def far_first(i):
    return NZ // 2 + jnp.where(lax.rem(i, 2) == 0, i // 2, -((i + 1) // 2))


def both(*conditions):
    out = conditions[0]
    for condition in conditions[1:]:
        out = jnp.logical_and(out, condition)
    return out


def neither(condition):
    return jnp.logical_not(condition)


def spread_rows(row):
    return jnp.broadcast_to(row, (8, PANEL))


def spread_lane(tile, lane):
    return jnp.broadcast_to(tile[:, lane:lane + 1], (8, PANEL))


def eliminate(groups, first, last, sub):
    for k in range(first, last, 4):
        g0, r0 = k // 8, k % 8
        head = groups[g0]
        rows = [[spread_rows(head[h][r0 + i:r0 + i + 1]) for h in range(2)] for i in range(4)]
        dots = [[spread_lane(rows[i][0], k + j) if j >= i else None for j in range(4)] for i in range(4)]
        mults = [[None] * 4 for _ in range(4)]
        scaled = []
        for i in range(4):
            inv = 1.0 / dots[i][i]
            for j in range(i + 1, 4):
                mults[i][j] = dots[i][j] * inv
            for j in range(i + 1, 4):
                for l in range(j, 4):
                    dots[j][l] = dots[j][l] - mults[i][j] * dots[i][l]
                rows[j] = [rows[j][h] - mults[i][j] * rows[i][h] for h in range(2)]
            scaled.append([rows[i][h] * inv for h in range(2)])
        for i in (2, 1, 0):
            for j in range(i + 1, 4):
                scaled[i] = [scaled[i][h] - mults[i][j] * scaled[j][h] for h in range(2)]
        for g in range(g0 if r0 == 0 else g0 + 1, PANEL // 8):
            tile = groups[g]
            new = list(tile)
            for j in range(4):
                factor = spread_lane(tile[0], k + j)
                new = [new[h] - factor * scaled[j][h] for h in range(2)]
            if g == g0:
                new = [jnp.where(sub > 3, new[h], tile[h]) for h in range(2)]
            groups[g] = new
        for h in range(2):
            tile = groups[g0][h]
            for i in range(4):
                tile = jnp.where(sub == r0 + i, rows[i][h], tile)
            groups[g0] = [tile, groups[g0][1]] if h == 0 else [groups[g0][0], tile]


def exchange(a_ref, out_ref, feats, slices, partial, inbox, total, pin, psum, tall, rows, cols, pivot, owned,
             tz, ty, tq, tr, square, hubs, strip, many, gram, gin, gpart, gx, gtot, block_in,
             g1_s, g1_r, sib_s, sib_r, sl_s, sl_r, z_s, z_r, tz_s, tz_r, ty_s, ty_r, p0_s, p0_r, p1_s, p1_r,
             rows_s, rows_r, cols_s, cols_r, piv_s, piv_r, own_s, own_r, move_s, move_r, hub_s, hub_r, gz_s, gz_r, gx_s, gx_r, gate, in_sem):
    x, z, y, c = (lax.axis_index(name) for name in ("x", "z", "y", "c"))
    other = 1 - c

    def along(d):
        return (x, lax.rem(z + d + NZ, NZ), y, c)

    def in_plane(i):
        return (lax.rem(x + i // (NY * NC), NX), z, lax.rem(y + i // NC, NY), lax.rem(c + i, NC))

    barrier = pltpu.get_barrier_semaphore()

    local(a_ref, block_in, in_sem)

    @pl.loop(1, PLANE)
    def _(i):
        pl.semaphore_signal(barrier, inc=1, device_id=in_plane(i), device_id_type=MESH)

    @pl.loop(1, NZ)
    def _(d):
        pl.semaphore_signal(barrier, inc=1, device_id=along(d), device_id_type=MESH)

    wait(block_in, in_sem)
    feats[c, x] = block_in[...].T
    pl.semaphore_wait(barrier, PLANE - 1 + NZ - 1)
    hub = both(y == 0, c == 0)
    panel = c == 0
    place = lax.rem(z + NZ - FIRST, NZ)
    holder = both(panel, place < STRIPS)
    place_s, place_h = place // NC, lax.rem(place, NC)

    def part(piece, h):
        return feats.at[c, piece, pl.ds(128 * h, 128)]

    def pass_on(piece, h, step, sem):
        send(part(piece, h), part(piece, h), g1_s.at[sem], g1_r.at[piece, h], (lax.rem(x + step, NX), z, y, c))

    def relay(piece, h):
        send(part(piece, h), part(piece, h), sib_s.at[piece], sib_r.at[piece], (x, z, y, other))
        parts = []
        for k in range(4 * h, 4 * h + 4):
            start = pl.multiple_of(32 * k + 16 * (x // 2), 16)
            tile = feats[c, piece, pl.ds(start, 16)].astype(F32)
            parts.append(jnp.where(lax.rem(x, 2) == 1, tile[8:], tile[:8]))
        slices[y, piece, pl.ds(32 * h, 32)] = jnp.concatenate(parts, axis=0).astype(BF16)
        for target in range(1, NY):
            @pl.when(target > y)
            def _():
                there = slices.at[y, piece, pl.ds(32 * h, 32)]
                send(there, there, sl_s.at[target, piece], sl_r.at[y, piece], (x, z, target, c))

    pass_on(x, 0, 1, 0)
    pass_on(x, 1, 3, 1)
    pass_on(x, 1, 1, 2)
    pass_on(x, 0, 3, 3)
    relay(x, 0)
    relay(x, 1)

    def gram_out():
        block = feats[c, x, :PANEL]
        block = lax.dot_general(block, block, (((1,), (1,)), ((), ())), preferred_element_type=F32)
        gram[...] = block.reshape(STRIPS, 16, PANEL)
        for n in range(STRIPS):
            target = (FIRST + n) % NZ
            pl.when(target == z)(lambda: local(gram.at[n], gin.at[z], gz_r))
            pl.when(target != z)(lambda: send(gram.at[n], gin.at[z], gz_s, gz_r, (x, target, y, c)))

    left_x, right_x, far_x = lax.rem(x + 3, NX), lax.rem(x + 1, NX), lax.rem(x + 2, NX)
    for i, (piece, h, step) in enumerate(
        ((left_x, 0, 1), (right_x, 1, 3), (left_x, 1, 0), (right_x, 0, 0), (far_x, 0, 0), (far_x, 1, 0))
    ):
        wait(part(piece, h), g1_r.at[piece, h])
        if step:
            pass_on(piece, h, step, 4 + h)
        relay(piece, h)
        if i == 0:
            pl.when(hub)(gram_out)

    @pl.when(both(hub, holder))
    def _():
        wait(gin, gz_r)
        gpart[...] = jnp.sum(gin[...], axis=0)
        for d in (1, 3, 2):
            send(gpart, gx.at[x], gx_s.at[d], gx_r, (lax.rem(x + d, NX), z, y, c))
        local(gpart, gx.at[x], gx_r)
    for piece in range(NX):
        wait(feats.at[other, piece], sib_r.at[piece])

    moved = {2: y == 3}
    taken = {2: y == 0}
    gets = z // STRIPS == c

    def owner_row(k):
        return jnp.where(taken[k], NY - 1 - y, y) if k in taken else y

    def active(k):
        own = k <= y
        return jnp.logical_or(both(own, neither(moved[k])), taken[k]) if k in moved else own

    def halved(k):
        return both(c == 1, y == k)

    def first_strip(k):
        return jnp.where(panel, 4, 0) if k == 0 else 0

    def receives(k):
        return both(gets, active(k), lax.rem(z, STRIPS) >= first_strip(k))

    def arrived(source):
        @pl.when(source < y)
        def _():
            for piece in range(NX):
                wait(slices.at[source, piece], sl_r.at[source, piece])

    def multiply(source):
        for half in range(NC):
            acc = jnp.zeros((SLICE, BLOCK), F32)
            for piece in range(NX):
                acc += lax.dot_general(slices[source, piece], feats[half, piece], (((1,), (1,)), ((), ())),
                                       preferred_element_type=F32)
            for s in range(STRIPS):
                partial[source, s, half] = acc[8 * s:8 * s + 8]

    def reduce_to_peers(ks, when):
        @pl.loop(0, NZ)
        def _(i):
            target = lax.rem(z + jnp.where(i == NZ - 1, 0, far_first(i)), NZ)
            s = lax.rem(target, STRIPS)
            for k in ks:
                src, dst = partial.at[k, s], inbox.at[k, z]
                fits = both(when(k), target // STRIPS == c, s >= first_strip(k))

                def go(src, dst):
                    pl.when(target == z)(lambda: local(src, dst, z_r.at[k]))
                    pl.when(target != z)(lambda: send(src, dst, z_s.at[k], z_r.at[k], (x, target, y, c)))

                pl.when(both(fits, neither(halved(k))))(lambda: go(src, dst))
                pl.when(both(fits, halved(k)))(lambda: go(src.at[1], dst.at[1]))

    def sent_to_peers(k):
        count = STRIPS - first_strip(k) - jnp.where(receives(k), 1, 0)
        for n in (3, 4, 7, 8):
            if n < 5 and k > 0:
                continue

            @pl.when(both(active(k), count == n, neither(halved(k))))
            def _():
                wait(partial.at[k, pl.ds(0, n)], z_s.at[k])

            @pl.when(both(active(k), count == n, halved(k)))
            def _():
                wait(partial.at[k, pl.ds(0, n), 1], z_s.at[k])

    def owners(k, act):
        for half in range(NC):
            needed = receives(k) if half == 1 else both(receives(k), neither(halved(k)))
            here = both(k == x, owner_row(k) == y, half == c)

            if act == "start":
                pl.when(both(needed, here))(lambda: local(total.at[k, half], owned.at[x], own_r))

            @pl.when(both(needed, neither(here)))
            def _():
                if act == "start":
                    send(total.at[k, half], owned.at[x], own_s.at[k, half], own_r, (k, z, owner_row(k), half))
                else:
                    wait(total.at[k, half], own_s.at[k, half])

    def reduced(k):
        @pl.when(both(receives(k), neither(halved(k))))
        def _():
            wait(inbox.at[k], z_r.at[k])
            total[k] = jnp.sum(inbox[k], axis=0)

        @pl.when(both(receives(k), halved(k)))
        def _():
            wait(inbox.at[k, :, 1], z_r.at[k])
            total[k, 1] = jnp.sum(inbox[k, :, 1], axis=0)
        owners(k, "start")

    def taken_in(k):
        if k in taken:
            @pl.when(taken[k])
            def _():
                wait(partial.at[k], move_r.at[k])

    arrived(0)
    multiply(0)

    @pl.when(panel)
    def _():
        for n in range(STRIPS):
            target = (FIRST + n) % NZ

            @pl.when(target == z)
            def _():
                local(partial.at[0, n // NC, n % NC], pin.at[z], p0_r)

            @pl.when(target != z)
            def _():
                send(partial.at[0, n // NC, n % NC], pin.at[z], p0_s, p0_r, (x, target, y, c))

    @pl.when(both(hub, holder))
    def _():
        wait(gx, gx_r)
        gtot[...] = jnp.sum(gx[...], axis=0)

        for d in (8, 7, 9, 6, 10, 5, 11, 4, 12, 3, 13, 2, 14, 1, 15):
            send(gtot, hubs.at[place], hub_s, hub_r, along(d))
        local(gtot, hubs.at[place], hub_r)

    tracer = both(x == NX - 1, c == 1)

    @pl.when(tracer)
    def _():
        acc = jnp.zeros((8, 128), F32)
        for half in range(NC):
            for piece in range(NX):
                v = feats[half, piece].astype(F32)
                v = jnp.sum((v * v).reshape(BLOCK // 8, 8, BLOCK), axis=0)
                acc += v[:, :128] + v[:, 128:]
        tq[...] = acc

        @pl.loop(0, NZ - 1)
        def _(d):
            send(tq, tz.at[z], tz_s, tz_r, along(far_first(d)))
        local(tq, tz.at[z], tz_r)

    for k in (2, 3, 1):
        @pl.when(k <= y)
        def _():
            arrived(k)
            multiply(k)
        if k in moved:
            @pl.when(moved[k])
            def _():
                send(partial.at[k], partial.at[k], move_s.at[k], move_r.at[k], (x, z, NY - 1 - y, c))

    def kept(k):
        return both(active(k), neither(taken[k])) if k in taken else active(k)

    pl.when(panel)(lambda: [reduce_to_peers((k,), kept) for k in (1, 0)] and None)

    @pl.when(holder)
    def _():
        wait(pin, p0_r)
        psum[...] = jnp.sum(pin[...], axis=0)

        for d in (8, 7, 9, 6, 10, 5, 11, 4, 12, 3, 13, 2, 14, 1, 15):
            send(psum, tall.at[place_h, place_s], p1_s, p1_r, along(d))
        local(psum, tall.at[place_h, place_s], p1_r)

    pl.when(panel)(lambda: reduce_to_peers((2, 3), kept))

    @pl.when(neither(panel))
    def _():
        for n in range(GATES):
            pl.semaphore_signal(gate.at[n], inc=1, device_id=along(8), device_id_type=MESH)
            pl.semaphore_wait(gate.at[n], 1)
        for k in range(NY):
            reduce_to_peers((k,), kept)

    taken_in(2)
    pl.when(taken[2])(lambda: reduce_to_peers((2,), active))

    @pl.when(tracer)
    def _():
        wait(tz, tz_r)
        tr[...] = jnp.sum(tz[...], axis=0)

        @pl.loop(1, PLANE)
        def _(i):
            send(tr, ty.at[y], ty_s, ty_r, in_plane(i))
        local(tr, ty.at[y], ty_r)

    @pl.when(hub)
    def _():
        wait(hubs, hub_r)

        @pl.loop(1, NY * NC)
        def _(i):
            send(hubs, pivot, piv_s.at[i], piv_r, (x, z, lax.rem(y + i // NC, NY), lax.rem(c + i, NC)))
        local(hubs, pivot, piv_r)

    def spread(src, dst, sems, recv, count, where, start):
        for i in range(count):
            tx, to_y, tc = where(i)
            here = both(tx == x, to_y == y, tc == c)
            if start:
                pl.when(here)(lambda: local(src, dst, recv))
                pl.when(neither(here))(lambda: send(src, dst, sems.at[i], recv, (tx, z, to_y, tc)))
            else:
                pl.when(neither(here))(lambda: wait(src, sems.at[i]))

    def spread_panel(start):
        spread(strip, cols.at[x], cols_s, cols_r, NY * NC, lambda i: (y, i // 2, lax.rem(i, NC)), start)
        for half in range(NC):
            spread(tall.at[half], rows.at[x], rows_s.at[half], rows_r, NX, lambda i: (lax.rem(x + i, NX), y, half), start)

    @pl.when(panel)
    def _():
        wait(tall, p1_r)
        mixed = tall[z // 8].reshape(32, BLOCK)
        mixed = jnp.where(lax.rem(z, 8) >= 4, mixed[:, 128:], mixed[:, :128])
        lanes = lax.broadcasted_iota(jnp.int32, (8, 128), 1) // 32
        packed = jnp.zeros((8, 128), F32)
        for q in range(4):
            turned = pltpu.roll(mixed[8 * q:8 * q + 8], lax.rem(32 * q - 32 * lax.rem(z, 4) + 128, 128), 1)
            packed = jnp.where(lanes == q, turned, packed)
        strip[...] = packed
        spread_panel(True)

    wait(pivot, piv_r)
    wait(ty, ty_r)
    damp = jnp.sum(jnp.sum(ty[...], axis=0), keepdims=True) * (SCALE * 0.01 / FULL)
    lane = lax.broadcasted_iota(jnp.int32, (8, PANEL), 1)
    sub = lax.broadcasted_iota(jnp.int32, (8, PANEL), 0)
    groups = []
    for g in range(PANEL // 8):
        diag = lane == sub + 8 * g
        left = pivot[g // 2, 8 * (g % 2):8 * (g % 2) + 8] * SCALE + jnp.where(diag, damp, 0.0)
        groups.append([left, jnp.where(diag, 1.0, 0.0).astype(F32)])
    eliminate(groups, 0, PANEL // 2, sub)
    for g in range(PANEL // 8):
        square[g, 0] = groups[g][0]
        square[g, 1] = groups[g][1]
    for k in range(NY):
        reduced(k)
    groups = [[square[g, 0], square[g, 1]] for g in range(PANEL // 8)]
    eliminate(groups, PANEL // 2, PANEL, sub)
    scaled = []
    for g in range(PANEL // 8):
        diag = jnp.sum(jnp.where(lane == sub + 8 * g, groups[g][0], 0.0), axis=1, keepdims=True)
        scaled.append(groups[g][1] * lax.rsqrt(diag))
    inverse = jnp.concatenate(scaled, axis=0)
    highest = lax.Precision.HIGHEST
    wait(cols, cols_r)
    left = jnp.concatenate([pltpu.roll(cols[i], (128 - 32 * q) % 128, 1) for q in range(4) for i in range(NX)], axis=0)
    left = jnp.dot(inverse, left * SCALE, precision=highest, preferred_element_type=F32)[:, :32]
    wait(rows, rows_r)
    ids = lax.broadcasted_iota(jnp.int32, (PANEL, BLOCK), 0)
    row0 = (y * NC + c) * BLOCK
    row_ids = row0 + lax.broadcasted_iota(jnp.int32, (PANEL, BLOCK), 1)
    right = jnp.concatenate([rows[i, q] for q in range(4) for i in range(NX)], axis=0)
    right = right * SCALE + jnp.where(ids == row_ids, damp, 0.0)
    right = jnp.dot(inverse, right, precision=highest, preferred_element_type=F32)
    update = lax.dot_general(left, right, (((0,), (0,)), ((), ())), precision=highest, preferred_element_type=F32)
    strip0 = (x * NZ + z) * 32
    leading = strip0 < PANEL
    wide = update
    for q in range(4):
        wide = jnp.where(both(leading, z == q), right[32 * q:32 * q + 32], wide)
    col_ids = strip0 + lax.broadcasted_iota(jnp.int32, (32, BLOCK), 0)
    row_ids = row0 + lax.broadcasted_iota(jnp.int32, (32, BLOCK), 1)

    @pl.when(both(neither(leading), NC * x + z // 8 <= NC * y + c))
    def _():
        wait(owned, own_r)
    schur = owned[...].reshape(32, BLOCK) * SCALE + jnp.where(col_ids == row_ids, damp, 0.0) - wide
    wide = jnp.where(leading, wide, schur)
    out_ref[...] = jnp.where(row_ids >= col_ids, wide, 0.0)

    for h in range(2):
        for sem in (0, 1, 2, 3, 4, 5):
            if sem in (0, 3) and h == 0 or sem in (1, 2) and h == 1 or sem == 4 + h:
                wait(part(x, h), g1_s.at[sem])
    for piece in range(NX):
        wait(feats.at[c, piece], sib_s.at[piece])
        for target in range(1, NY):
            @pl.when(target > y)
            def _():
                wait(slices.at[y, piece], sl_s.at[target, piece])
    for k in range(NY):
        sent_to_peers(k)
        owners(k, "finish")
    for k in moved:
        @pl.when(moved[k])
        def _():
            wait(partial.at[k], move_s.at[k])

    @pl.when(tracer)
    def _():
        wait(tz.at[pl.ds(0, NZ - 1)], tz_s)
        wait(many.at[pl.ds(0, PLANE - 1)], ty_s)

    @pl.when(hub)
    def _():
        @pl.loop(1, NY * NC)
        def _(i):
            wait(hubs, piv_s.at[i])

    @pl.when(holder)
    def _():
        wait(pin.at[pl.ds(0, STRIPS - 1)], p0_s)
        wait(pin.at[pl.ds(0, NZ - 1)], p1_s)

    @pl.when(both(hub, holder))
    def _():
        wait(gram.at[pl.ds(0, STRIPS - 1)], gz_s)
        for d in (1, 3, 2):
            wait(gpart, gx_s.at[d])
        wait(gin.at[pl.ds(0, NZ - 1)], hub_s)

    @pl.when(both(hub, neither(holder)))
    def _():
        wait(gram, gz_s)

    @pl.when(both(panel, neither(holder)))
    def _():
        wait(pin.at[pl.ds(0, STRIPS)], p0_s)
    pl.when(panel)(lambda: spread_panel(False))


def shards(a):
    dma = pltpu.SemaphoreType.DMA
    vmem = pl.BlockSpec(memory_space=pltpu.VMEM)
    result = pl.pallas_call(
        exchange,
        out_shape=jax.ShapeDtypeStruct((32, BLOCK), F32),
        in_specs=[pl.BlockSpec(memory_space=pl.ANY)],
        out_specs=vmem,
        scratch_shapes=[
            pltpu.VMEM((NC, NX, BLOCK, BLOCK), BF16),
            pltpu.VMEM((NY, NX, SLICE, BLOCK), BF16),
            pltpu.VMEM((NY, STRIPS, NC, 8, BLOCK), F32),
            pltpu.VMEM((NY, NZ, NC, 8, BLOCK), F32),
            pltpu.VMEM((NY, NC, 8, BLOCK), F32),
            pltpu.VMEM((NZ, 8, BLOCK), F32),
            pltpu.VMEM((8, BLOCK), F32),
            pltpu.VMEM((NC, 4, 8, BLOCK), F32),
            pltpu.VMEM((NX, 4, 8, BLOCK), F32),
            pltpu.VMEM((NX, 8, 128), F32),
            pltpu.VMEM((STRIPS, 16, 128), F32),
            pltpu.VMEM((NX, 8, BLOCK), F32),
            pltpu.VMEM((NZ, 8, 128), F32),
            pltpu.VMEM((NY, 8, 128), F32),
            pltpu.VMEM((8, 128), F32),
            pltpu.VMEM((8, 128), F32),
            pltpu.VMEM((PANEL // 8, 2, 8, PANEL), F32),
            pltpu.VMEM((STRIPS, 16, 128), F32),
            pltpu.VMEM((8, 128), F32),
            pltpu.VMEM((PLANE, 8, 128), F32),
            pltpu.VMEM((STRIPS, 16, 128), F32),
            pltpu.VMEM((NZ, 16, 128), F32),
            pltpu.VMEM((16, 128), F32),
            pltpu.VMEM((NX, 16, 128), F32),
            pltpu.VMEM((16, 128), F32),
            pltpu.VMEM((BLOCK, BLOCK), BF16),
            dma((6,)), dma((NX, 2)),
            dma((NX,)), dma((NX,)),
            dma((NY, NX)), dma((NY, NX)),
            dma((NY,)), dma((NY,)),
            dma(()), dma(()),
            dma(()), dma(()),
            dma(()), dma(()),
            dma(()), dma(()),
            dma((NC, NX)), dma(()),
            dma((NY * NC,)), dma(()),
            dma((NY * NC,)), dma(()),
            dma((NY, NC)), dma(()),
            dma((NY,)), dma((NY,)),
            dma(()), dma(()),
            dma(()), dma(()),
            dma((NX,)), dma(()),
            pltpu.SemaphoreType.REGULAR((1,)),
            dma(()),
        ],
        compiler_params=pltpu.CompilerParams(collective_id=0, has_side_effects=True),
    )(a)
    return result.T


def solution(mesh):
    finer = Mesh(mesh.devices.reshape(NX, NZ, NY, NC), ("x", "z", "y", "c"))
    return jax.shard_map(
        shards, mesh=finer, in_specs=(P(("x", "z"), ("y", "c")),), out_specs=P(("y", "c"), ("x", "z")), check_vma=False
    )
```
